32 devices in a mesh: ba: 8 (over y, x, core), col: 4 (over z).
Axes of the slice: x: 2, y: 2, z: 4, core: 2. Of those that a mesh axis runs over, the one named last changes fastest.
Arguments:
- r_pairs: bfloat16 [1, 3, 512, 512], replicated, may hold values from -6 to 6
- w_tiles: bfloat16 [1, 3, 512, 512, 512], P(None, None, 'ba', 'col'), may hold values from -0.375 to 0.375
- virt_energy: float32 [512], replicated, may hold values from 0.3 to 3
- energy_shift: float32 [1], replicated, may hold values from -14 to -8
Outputs:
- sigma: float32 [1, 3, 512, 512], P(None, None, 'ba', 'col')
The draws below stay inside these ranges and needn't reach their ends.
All inputs are finite; a program needn't handle non-finite values.
Results may differ from the reference program's by a relative error of at most 0.00077.
Values may be sent and summed in bfloat16 or wider, within the bound.
A program may use at most 128 MiB of HBM per device.

```python
import jax
import jax.numpy as jnp
from jax import lax

V = 512
TRIPLES = 1


def spiked(drawn, own_key, source, target, blocks, factor):
    owner, partner = [(jnp.arange(drawn.shape[dim]) // (drawn.shape[dim] // blocks)).reshape([-1 if axis == dim else 1 for axis in range(drawn.ndim)]) for dim in (source, target)]
    chosen = jax.random.permutation(own_key, blocks)[partner]
    strong = (owner == chosen) | (owner == (partner + blocks // 2) % blocks)
    return jnp.where(strong, factor * drawn, drawn)


def levels(key, extent, shards, smallest, top_value):
    factor_of, own = 1.0, jax.random.fold_in(key, 6)
    for position, parts in shards:
        steps = jnp.exp(jax.random.uniform(jax.random.fold_in(own, position), (parts,), jnp.float32, smallest / len(shards), top_value / len(shards)))
        factor_of = factor_of * jnp.repeat(steps, extent[position] // parts).reshape([-1 if axis == position else 1 for axis in range(len(extent))])
    return factor_of


def noise(stream_key, dims, deviation, most, shards=(), kind=jnp.bfloat16):
    drawn = deviation * jax.random.normal(stream_key, dims, jnp.float32)
    if shards:
        drawn = drawn * levels(stream_key, dims, shards, -0.22, 0.18)
    return jnp.clip(drawn, -most, most).astype(kind)


def heavy_noise(stream_key, extent, scale, reach, shards, heavy, dtype=jnp.bfloat16):
    result = scale * jax.random.normal(stream_key, extent, jnp.float32)
    if shards:
        result = result * levels(stream_key, extent, shards, -0.22, 0.18)
    return jnp.clip(spiked(result, jax.random.fold_in(stream_key, 3), *heavy), -reach, reach).astype(dtype)


def setup_inputs(seed: int = 0) -> dict:
    key_list = jax.random.split(jax.random.key(seed), 5)
    return {
        "r_pairs": noise(key_list[0], (TRIPLES, 3, V, V), 1.0, 6.0),
        "w_tiles": heavy_noise(key_list[1], (TRIPLES, 3, V, V, V), V ** -0.5, 0.375, ((2, 8), (3, 4)), (3, 4, 4, 2.0)),
        "virt_energy": jnp.clip(jax.random.uniform(key_list[2], (V,), jnp.float32, 0.3, 3.0), 0.3, 3.0),
        "energy_shift": jnp.clip(jax.random.uniform(key_list[3], (TRIPLES,), jnp.float32, -14.0, -8.0), -14.0, -8.0),
    }


def one_triple(inputs):
    rows, tiles, shift_value = inputs
    flat = tiles.reshape(3, V * V, V)
    cubes = jnp.dot(rows[0], flat[0].T, preferred_element_type=jnp.float32)
    cubes = cubes + jnp.dot(rows[1], flat[1].T, preferred_element_type=jnp.float32)
    cubes = cubes + jnp.dot(rows[2], flat[2].T, preferred_element_type=jnp.float32)
    cubes = cubes.astype(jnp.bfloat16).reshape(V, V, V)
    bc_summed = (cubes.astype(jnp.float32) + jnp.swapaxes(cubes, 1, 2).astype(jnp.float32)).astype(jnp.bfloat16)
    return bc_summed, flat, shift_value


def reference(r_pairs, w_tiles, virt_energy, energy_shift):
    def finish(inputs):
        bc_summed, flat, shift_value = one_triple(inputs)
        combined = bc_summed.astype(jnp.float32) + jnp.swapaxes(bc_summed, 0, 1).astype(jnp.float32)
        denominator = shift_value - virt_energy[:, None, None] - virt_energy[None, :, None] - virt_energy[None, None, :]
        combined = (combined / denominator).astype(jnp.bfloat16).reshape(V, V * V)
        blocks = [jnp.dot(combined, flat[which], preferred_element_type=jnp.float32) for which in range(3)]
        return jnp.stack(blocks)

    return lax.map(finish, (r_pairs, w_tiles, energy_shift))
```

```python
import functools

import jax
import jax.numpy as jnp
from jax import lax
from jax.experimental import pallas as pl
from jax.experimental.pallas import tpu as pltpu
from jax.sharding import PartitionSpec as P

MESH = pl.DeviceIdType.MESH
CHUNKS = 8


def scatter_sum(blocks, axis, order):
    count = blocks.shape[0]
    bits = count.bit_length() - 1
    me = lax.axis_index(axis)
    payload = blocks.shape[1:]
    left = list(range(bits))[::-1]
    blocks = blocks.reshape([2] * bits + list(payload))
    for bit in order:
        place = left.index(bit)
        own = jnp.bitwise_and(jnp.right_shift(me, bit), 1)
        kept = lax.dynamic_index_in_dim(blocks, own, place, keepdims=False)
        given = lax.dynamic_index_in_dim(blocks, 1 - own, place, keepdims=False)
        swap = [(n, n ^ (1 << bit)) for n in range(count)]
        blocks = kept + lax.ppermute(given, axis, swap)
        left.remove(bit)
    return blocks


def exchange_kernel(
    nb, nc, chunks, cube, base_a, energy_b, energy_c, out, slab, turned, summed, home, out_sems, in_sems, own_sems
):
    rows, bw, cw = slab.shape[2:]
    ratio = nb // nc
    b_me, c_me = lax.axis_index("ba"), lax.axis_index("col")
    barrier = pltpu.get_barrier_semaphore()
    for step in range(1, nb):
        pl.semaphore_signal(barrier, inc=1, device_id=(b_me ^ step, c_me), device_id_type=MESH)
    for step in range(1, nc):
        pl.semaphore_signal(barrier, inc=1, device_id=(b_me, c_me ^ step), device_id_type=MESH)
    pl.semaphore_wait(barrier, nb + nc - 2)

    def spread(chunk):
        for step in range(1, nb):
            pltpu.make_async_remote_copy(
                src_ref=cube.at[b_me ^ step, chunk],
                dst_ref=slab.at[chunk, b_me],
                send_sem=out_sems.at[0, chunk],
                recv_sem=in_sems.at[0, chunk],
                device_id=(b_me ^ step, c_me),
                device_id_type=MESH,
            ).start()

    def own_slab(chunk):
        return pltpu.make_async_copy(cube.at[b_me, chunk], slab.at[chunk, b_me], own_sems.at[0, chunk])

    def own_turned(chunk):
        return pltpu.make_async_copy(
            slab.at[chunk, pl.ds(c_me * ratio, ratio)], turned.at[chunk, c_me], own_sems.at[1, chunk]
        )

    def own_home(chunk):
        return pltpu.make_async_copy(summed.at[chunk, b_me], home.at[chunk, b_me], own_sems.at[2, chunk])

    def turn(chunk):
        for step in range(1, nc):
            level = c_me ^ step
            pltpu.make_async_remote_copy(
                src_ref=slab.at[chunk, pl.ds(level * ratio, ratio)],
                dst_ref=turned.at[chunk, c_me],
                send_sem=out_sems.at[1, chunk],
                recv_sem=in_sems.at[1, chunk],
                device_id=(b_me, level),
                device_id_type=MESH,
            ).start()

    def back(chunk):
        for step in range(1, nb):
            pltpu.make_async_remote_copy(
                src_ref=summed.at[chunk, b_me ^ step],
                dst_ref=home.at[chunk, b_me],
                send_sem=out_sems.at[2, chunk],
                recv_sem=in_sems.at[2, chunk],
                device_id=(b_me ^ step, c_me),
                device_id_type=MESH,
            ).start()

    buffers = (slab, turned, home)
    peers = (nb - 1, nc - 1, nb - 1)

    def arrived(kind, chunk):
        whole = buffers[kind].at[chunk, pl.ds(0, peers[kind])]
        pltpu.make_async_copy(whole, whole, in_sems.at[kind, chunk]).wait()

    def left(kind, chunk):
        whole = buffers[kind].at[chunk, pl.ds(0, peers[kind])]
        pltpu.make_async_copy(whole, whole, out_sems.at[kind, chunk]).wait()

    def add(chunk):
        @pl.loop(0, rows)
        def _(row):
            for level in range(nc):
                whole = jnp.concatenate([turned[chunk, level, part, row] for part in range(ratio)], 0)
                flipped = whole.astype(jnp.float32).T
                for part in range(ratio):
                    block = level * ratio + part
                    kept = slab[chunk, block, row].astype(jnp.float32)
                    total = kept + flipped[part * bw : (part + 1) * bw]
                    summed[chunk, block, row] = total.astype(jnp.bfloat16)

    @pl.loop(0, chunks)
    def _(chunk):
        spread(chunk)
        own_slab(chunk).start()

    @pl.loop(0, chunks)
    def _(chunk):
        arrived(0, chunk)
        own_slab(chunk).wait()
        turn(chunk)
        own_turned(chunk).start()

        @pl.when(chunk > 0)
        def _():
            arrived(1, chunk - 1)
            own_turned(chunk - 1).wait()
            add(chunk - 1)
            back(chunk - 1)
            own_home(chunk - 1).start()

    arrived(1, chunks - 1)
    own_turned(chunks - 1).wait()
    add(chunks - 1)
    back(chunks - 1)
    own_home(chunks - 1).start()

    @pl.loop(0, chunks)
    def _(chunk):
        for kind in range(3):
            left(kind, chunk)
        arrived(2, chunk)
        own_home(chunk).wait()

    a_tile = min(16, bw)
    b_tile = min(16, bw)
    a_steps, b_steps = bw // a_tile, bw // b_tile
    row_c = energy_c[...]

    def pieces(ref, tile, index, block, inner):
        if tile >= rows:
            count = tile // rows
            return jnp.concatenate([ref[index * count + n, block, :, inner, :] for n in range(count)], 0)
        part = rows // tile
        return ref[index // part, block, pl.ds((index % part) * tile, tile), inner, :]

    @pl.loop(0, nb * a_steps * b_steps)
    def _(place):
        block = place // (a_steps * b_steps)
        a_step = (place // b_steps) % a_steps
        b_step = place % b_steps
        a_inner = pl.ds(pl.multiple_of(a_step * a_tile, a_tile), a_tile)
        b_inner = pl.ds(pl.multiple_of(b_step * b_tile, b_tile), b_tile)
        mine = pieces(summed, b_tile, b_step, block, a_inner).astype(jnp.float32)
        theirs = pieces(home, a_tile, a_step, block, b_inner).astype(jnp.float32)
        total = mine + jnp.swapaxes(theirs, 0, 1)
        a_rows = pl.ds(pl.multiple_of(block * bw + a_step * a_tile, a_tile), a_tile)
        base = base_a[a_rows, :]
        for b in range(b_tile):
            below = base - energy_b[b_step * b_tile + b] - row_c
            out[b_step * b_tile + b, a_rows, :] = (total[b] / below).astype(jnp.bfloat16)


def combine(cubes, base_a, energy_b, energy_c, nb, nc):
    width, bw, cw = nb * cubes.shape[3], cubes.shape[3], cubes.shape[4]
    chunks = cubes.shape[1]
    rows = bw // chunks
    block = (rows, bw, cw)
    bf16 = jnp.bfloat16
    vmem = pl.BlockSpec(memory_space=pltpu.VMEM)
    return pl.pallas_call(
        functools.partial(exchange_kernel, nb, nc, chunks),
        out_shape=jax.ShapeDtypeStruct((bw, width, cw), bf16),
        in_specs=[
            pl.BlockSpec(memory_space=pl.ANY),
            vmem,
            pl.BlockSpec(memory_space=pltpu.SMEM),
            vmem,
        ],
        out_specs=vmem,
        scratch_shapes=[
            pltpu.VMEM((chunks, nb) + block, bf16),
            pltpu.VMEM((chunks, nc, nb // nc) + block, bf16),
            pltpu.VMEM((chunks, nb) + block, bf16),
            pltpu.VMEM((chunks, nb) + block, bf16),
            pltpu.SemaphoreType.DMA((3, chunks)),
            pltpu.SemaphoreType.DMA((3, chunks)),
            pltpu.SemaphoreType.DMA((3, chunks)),
        ],
        compiler_params=pltpu.CompilerParams(
            collective_id=0, has_side_effects=True, vmem_limit_bytes=56 << 20
        ),
    )(cubes, base_a, energy_b, energy_c)


def on_device(r_pairs, w_tiles, virt_energy, energy_shift):
    width = w_tiles.shape[4]
    bw, cw = w_tiles.shape[2], w_tiles.shape[3]
    nb, nc = lax.axis_size("ba"), lax.axis_size("col")
    energy_b = lax.dynamic_slice_in_dim(virt_energy, lax.axis_index("ba") * bw, bw)
    energy_c = lax.dynamic_slice_in_dim(virt_energy, lax.axis_index("col") * cw, cw)
    base_a = jnp.broadcast_to((energy_shift - virt_energy)[:, None], (width, cw))
    flat = w_tiles.reshape(3, bw * cw, width)
    cubes = jnp.einsum("mad,mxd->ax", r_pairs[0], flat, preferred_element_type=jnp.float32)
    chunks = min(CHUNKS, bw)
    cubes = cubes.astype(jnp.bfloat16).reshape(nb, chunks, bw // chunks, bw, cw)
    combined = combine(cubes, base_a, energy_b, energy_c[None], nb, nc)
    partial_sum = jnp.einsum(
        "bac,mbcd->mad", combined, w_tiles[0], preferred_element_type=jnp.float32
    )
    bits = list(range(nb.bit_length() - 1))
    split = partial_sum.reshape(3, nb, 2, bw // 2, width)
    halves = []
    for half, order in enumerate((bits, bits[:1] + bits[:0:-1])):
        part = scatter_sum(jnp.swapaxes(split[:, :, half], 0, 1), "ba", order)
        part = part.reshape(3, bw // 2, nc, cw)
        halves.append(scatter_sum(jnp.moveaxis(part, 2, 0), "col", list(range(nc.bit_length() - 1))[::-1]))
    return jnp.concatenate(halves, 1)[None]


def solution(mesh):
    in_specs = (P(), P(None, None, "ba", "col", None), P(), P())
    out_specs = P(None, None, "ba", "col")
    return jax.shard_map(
        on_device, mesh=mesh, in_specs=in_specs, out_specs=out_specs, check_vma=False
    )
```

```python
import functools

import jax
import jax.numpy as jnp
from jax import lax
from jax.experimental import pallas as pl
from jax.experimental.pallas import tpu as pltpu
from jax.sharding import PartitionSpec as P

MESH = pl.DeviceIdType.MESH
CHUNKS = 8
GROUP = 16
SLOTS = 4
LANES = 128
BF16, F32 = jnp.bfloat16, jnp.float32


def whole_kernel(nb, nc, chunks, *refs):
    cube, w_tiles, base_a, energy_b, energy_c, sigma = refs[:6]
    slab, turned, summed, home, combined, w_slots, total = refs[6:13]
    halved, dealt, spread_out = refs[13:-8], refs[-8], refs[-7]
    out_sems, in_sems, own_sems, w_sems, send_sems, got_sems = refs[-6:]
    rows, bw, cw = slab.shape[2:]
    width = nb * bw
    ratio = nb // nc
    bits = nb.bit_length() - 1
    b_me, c_me = lax.axis_index("ba"), lax.axis_index("col")
    barrier = pltpu.get_barrier_semaphore()
    for step in range(1, nb):
        pl.semaphore_signal(barrier, inc=1, device_id=(b_me ^ step, c_me), device_id_type=MESH)
    for step in range(1, nc):
        pl.semaphore_signal(barrier, inc=1, device_id=(b_me, c_me ^ step), device_id_type=MESH)
    pl.semaphore_wait(barrier, nb + nc - 2)

    def spread(chunk):
        for step in range(1, nb):
            pltpu.make_async_remote_copy(
                src_ref=cube.at[b_me ^ step, chunk],
                dst_ref=slab.at[chunk, b_me],
                send_sem=out_sems.at[0, chunk],
                recv_sem=in_sems.at[0, chunk],
                device_id=(b_me ^ step, c_me),
                device_id_type=MESH,
            ).start()

    def own_slab(chunk):
        return pltpu.make_async_copy(cube.at[b_me, chunk], slab.at[chunk, b_me], own_sems.at[0, chunk])

    def own_turned(chunk):
        return pltpu.make_async_copy(
            slab.at[chunk, pl.ds(c_me * ratio, ratio)], turned.at[chunk, c_me], own_sems.at[1, chunk]
        )

    def own_home(chunk):
        return pltpu.make_async_copy(summed.at[chunk, b_me], home.at[chunk, b_me], own_sems.at[2, chunk])

    def turn(chunk):
        for step in range(1, nc):
            level = c_me ^ step
            pltpu.make_async_remote_copy(
                src_ref=slab.at[chunk, pl.ds(level * ratio, ratio)],
                dst_ref=turned.at[chunk, c_me],
                send_sem=out_sems.at[1, chunk],
                recv_sem=in_sems.at[1, chunk],
                device_id=(b_me, level),
                device_id_type=MESH,
            ).start()

    def back(chunk):
        for step in range(1, nb):
            pltpu.make_async_remote_copy(
                src_ref=summed.at[chunk, b_me ^ step],
                dst_ref=home.at[chunk, b_me],
                send_sem=out_sems.at[2, chunk],
                recv_sem=in_sems.at[2, chunk],
                device_id=(b_me ^ step, c_me),
                device_id_type=MESH,
            ).start()

    buffers = (slab, turned, home)
    peers = (nb - 1, nc - 1, nb - 1)

    def arrived(kind, chunk):
        whole = buffers[kind].at[chunk, pl.ds(0, peers[kind])]
        pltpu.make_async_copy(whole, whole, in_sems.at[kind, chunk]).wait()

    def left(kind, chunk):
        whole = buffers[kind].at[chunk, pl.ds(0, peers[kind])]
        pltpu.make_async_copy(whole, whole, out_sems.at[kind, chunk]).wait()

    def add(chunk):
        @pl.loop(0, rows)
        def _(row):
            for level in range(nc):
                other = jnp.concatenate([turned[chunk, level, part, row] for part in range(ratio)], 0)
                flipped = other.astype(F32).T
                for part in range(ratio):
                    block = level * ratio + part
                    kept = slab[chunk, block, row].astype(F32)
                    summed[chunk, block, row] = (kept + flipped[part * bw : (part + 1) * bw]).astype(BF16)

    per = GROUP // rows
    steps = bw // GROUP
    row_c = energy_c[...]
    pack = max(1, LANES // cw)

    def gathered(ref, index, block, inner):
        return jnp.concatenate([ref[index * per + n, block, :, inner, :] for n in range(per)], 0)

    def combine(a_step, b_step, block):
        a_inner = pl.ds(pl.multiple_of(a_step * GROUP, GROUP), GROUP)
        b_inner = pl.ds(pl.multiple_of(b_step * GROUP, GROUP), GROUP)
        mine = gathered(summed, b_step, block, a_inner).astype(F32)
        theirs = gathered(home, a_step, block, b_inner).astype(F32)
        both = mine + jnp.swapaxes(theirs, 0, 1)
        a_rows = pl.ds(pl.multiple_of(block * bw + a_step * GROUP, GROUP), GROUP)
        base = base_a[a_rows, :]
        for b in range(0, GROUP, pack):
            place = b_step * GROUP + b
            entries = [both[b + n] / (base - energy_b[place + n] - row_c) for n in range(pack)]
            lanes = pl.ds(pl.multiple_of(place * cw, pack * cw), pack * cw)
            combined[a_rows, lanes] = jnp.concatenate(entries, 1).astype(BF16)

    def widen(step):
        for n in range(per):
            arrived(2, step * per + n)
            own_home(step * per + n).wait()

        @pl.loop(0, (2 * step + 1) * nb)
        def _(place):
            cell, block = place // nb, place % nb
            a_step = jnp.where(cell <= step, step, cell - step - 1)
            b_step = jnp.where(cell <= step, cell, step)
            combine(a_step, b_step, block)

    part_width = width // 2
    units = 6
    tiles = bw // GROUP
    depth = GROUP * cw

    def fetch(index):
        unit, tile = index // tiles, index % tiles
        slot = index % SLOTS
        return pltpu.make_async_copy(
            w_tiles.at[
                0,
                unit // 2,
                pl.ds(tile * GROUP, GROUP),
                :,
                pl.ds(pl.multiple_of((unit % 2) * part_width, part_width), part_width),
            ],
            w_slots.at[slot],
            w_sems.at[slot],
        )

    def product(unit):
        where = [unit // 2] + [slice(None)] * bits + [slice(None), pl.ds((unit % 2) * part_width, part_width)]

        @pl.loop(0, tiles)
        def _(tile):
            index = unit * tiles + tile
            fetch(index).wait()
            entries = combined[:, pl.ds(pl.multiple_of(tile * depth, depth), depth)]
            piece = jnp.dot(
                entries, w_slots[index % SLOTS].reshape(depth, part_width), preferred_element_type=F32
            ).reshape([2] * bits + [bw, part_width])

            @pl.when(tile == 0)
            def _():
                total[tuple(where)] = piece

            @pl.when(tile > 0)
            def _():
                total[tuple(where)] = total[tuple(where)] + piece

            @pl.when(index + SLOTS < units * tiles)
            def _():
                fetch(index + SLOTS).start()

    def bit(place):
        return (b_me // (1 << place)) % 2

    def order(unit):
        return list(range(bits)) if unit % 2 == 0 else [0] + list(range(1, bits))[::-1]

    def region(unit, fixed):
        lanes = pl.ds((unit % 2) * part_width, part_width)
        picks = [fixed.get(place, slice(None)) for place in range(bits)[::-1]]
        return tuple([unit // 2] + picks + [slice(None), lanes])

    def halving(unit, stage):
        done = order(unit)[:stage]
        place = order(unit)[stage]
        fixed = {n: bit(n) for n in done}
        fixed[place] = 1 - bit(place)
        return pltpu.make_async_remote_copy(
            src_ref=total.at[region(unit, fixed)],
            dst_ref=halved[stage].at[unit],
            send_sem=send_sems.at[unit, stage],
            recv_sem=got_sems.at[unit, stage],
            device_id=(b_me ^ (1 << place), c_me),
            device_id_type=MESH,
        )

    def halved_add(unit, stage):
        halving(unit, stage).wait_recv()
        where = region(unit, {n: bit(n) for n in order(unit)[: stage + 1]})
        total[where] = total[where] + halved[stage][unit]

    levels = nc // 2

    def deal(unit, n):
        level = (unit % 2) * levels + n
        return level, pltpu.make_async_remote_copy(
            src_ref=dealt.at[unit, n],
            dst_ref=spread_out.at[unit // 2, c_me],
            send_sem=send_sems.at[unit, bits + n],
            recv_sem=got_sems.at[unit // 2, bits],
            device_id=(b_me, level),
            device_id_type=MESH,
        )

    def deal_blocks(unit):
        block = total[region(unit, {place: bit(place) for place in range(bits)})]
        for n in range(levels):
            dealt[unit, n] = block[:, n * cw : (n + 1) * cw]

    def deal_start(unit):
        for n in range(levels):
            level, copy = deal(unit, n)
            pl.when(level != c_me)(copy.start)

    def deal_sent(unit):
        for n in range(levels):
            level, copy = deal(unit, n)
            pl.when(level != c_me)(copy.wait_send)

    def finish(unit):
        @pl.when(c_me // levels == unit % 2)
        def _():
            landed = spread_out.at[unit // 2, pl.ds(0, nc - 1)]
            pltpu.make_async_copy(landed, landed, got_sems.at[unit // 2, bits]).wait()
            result = dealt[unit, c_me % levels]
            for step in range(1, nc):
                result = result + spread_out[unit // 2, c_me ^ step]
            sigma[unit // 2] = result

    for index in range(SLOTS):
        fetch(index).start()

    @pl.loop(0, chunks)
    def _(chunk):
        spread(chunk)
        own_slab(chunk).start()

    def settle(chunk):
        arrived(1, chunk)
        own_turned(chunk).wait()
        add(chunk)
        back(chunk)
        own_home(chunk).start()

    for chunk in range(chunks):
        arrived(0, chunk)
        own_slab(chunk).wait()
        turn(chunk)
        own_turned(chunk).start()
        if chunk > 0:
            settle(chunk - 1)
        early = steps - chunks + chunk - 1
        if early >= 0:
            widen(early)
    settle(chunks - 1)
    widen(steps - 1)

    for time in range(units + bits + 1):
        if time < units:
            product(time)
        for stage in range(bits):
            if 0 <= time - stage - 1 < units:
                halved_add(time - stage - 1, stage)
        if 0 <= time - bits < units:
            deal_blocks(time - bits)
        for stage in range(bits):
            if 0 <= time - stage < units:
                halving(time - stage, stage).start()
        if 0 <= time - bits < units:
            deal_start(time - bits)
        if 0 <= time - bits - 1 < units:
            finish(time - bits - 1)
    for unit in range(units):
        for stage in range(bits):
            halving(unit, stage).wait_send()
        deal_sent(unit)

    @pl.loop(0, chunks)
    def _(chunk):
        for kind in range(3):
            left(kind, chunk)


def doubles(cubes, w_tiles, base_a, energy_b, energy_c, nb, nc):
    chunks, rows, bw, cw = cubes.shape[1:]
    width = nb * bw
    bits = nb.bit_length() - 1
    block = (rows, bw, cw)
    vmem = pl.BlockSpec(memory_space=pltpu.VMEM)
    hbm = pl.BlockSpec(memory_space=pl.ANY)
    return pl.pallas_call(
        functools.partial(whole_kernel, nb, nc, chunks),
        out_shape=jax.ShapeDtypeStruct((3, bw, cw), F32),
        in_specs=[hbm, hbm, vmem, pl.BlockSpec(memory_space=pltpu.SMEM), vmem],
        out_specs=vmem,
        scratch_shapes=[
            pltpu.VMEM((chunks, nb) + block, BF16),
            pltpu.VMEM((chunks, nc, nb // nc) + block, BF16),
            pltpu.VMEM((chunks, nb) + block, BF16),
            pltpu.VMEM((chunks, nb) + block, BF16),
            pltpu.VMEM((width, bw * cw), BF16),
            pltpu.VMEM((SLOTS, GROUP, cw, width // 2), BF16),
            pltpu.VMEM((3,) + (2,) * bits + (bw, width), F32),
        ]
        + [pltpu.VMEM((6,) + (2,) * (bits - 1 - stage) + (bw, width // 2), F32) for stage in range(bits)]
        + [
            pltpu.VMEM((6, nc // 2, bw, cw), F32),
            pltpu.VMEM((3, nc, bw, cw), F32),
            pltpu.SemaphoreType.DMA((3, chunks)),
            pltpu.SemaphoreType.DMA((3, chunks)),
            pltpu.SemaphoreType.DMA((3, chunks)),
            pltpu.SemaphoreType.DMA((SLOTS,)),
            pltpu.SemaphoreType.DMA((6, bits + nc // 2)),
            pltpu.SemaphoreType.DMA((6, bits + 1)),
        ],
        compiler_params=pltpu.CompilerParams(
            collective_id=0, has_side_effects=True, vmem_limit_bytes=60 << 20
        ),
    )(cubes, w_tiles, base_a, energy_b, energy_c)


def on_device(r_pairs, w_tiles, virt_energy, energy_shift):
    width = w_tiles.shape[4]
    bw, cw = w_tiles.shape[2], w_tiles.shape[3]
    nb, nc = lax.axis_size("ba"), lax.axis_size("col")
    energy_b = lax.dynamic_slice_in_dim(virt_energy, lax.axis_index("ba") * bw, bw)
    energy_c = lax.dynamic_slice_in_dim(virt_energy, lax.axis_index("col") * cw, cw)
    base_a = jnp.broadcast_to((energy_shift - virt_energy)[:, None], (width, cw))
    flat = w_tiles.reshape(3, bw * cw, width)
    cubes = jnp.einsum("mad,mxd->ax", r_pairs[0], flat, preferred_element_type=F32)
    cubes = cubes.astype(BF16).reshape(nb, CHUNKS, bw // CHUNKS, bw, cw)
    return doubles(cubes, w_tiles, base_a, energy_b, energy_c[None], nb, nc)[None]


def solution(mesh):
    in_specs = (P(), P(None, None, "ba", "col", None), P(), P())
    out_specs = P(None, None, "ba", "col")
    return jax.shard_map(
        on_device, mesh=mesh, in_specs=in_specs, out_specs=out_specs, check_vma=False
    )
```

```python
import functools

import jax
import jax.numpy as jnp
from jax import lax
from jax.experimental import pallas as pl
from jax.experimental.pallas import tpu as pltpu
from jax.sharding import PartitionSpec as P

MESH = pl.DeviceIdType.MESH
CHUNKS = 8
GROUP = 16
HALF = 8
TURNS = 3
FIRST = 64
BF16, F32 = jnp.bfloat16, jnp.float32


def whole_kernel(nb, nc, chunks, *refs):
    r_rows, w_tiles, base_a, energy_b, energy_c, sigma = refs[:6]
    slab, turned, summed, home, pool, w_slots, raw, total = refs[6:14]
    halved, dealt, spread_out = refs[14:-8], refs[-8], refs[-7]
    out_sems, in_sems, own_sems, w_sems, send_sems, got_sems = refs[-6:]
    rows, bw, cw = slab.shape[2:]
    width = nb * bw
    ratio = nb // nc
    bits = nb.bit_length() - 1
    b_me, c_me = lax.axis_index("ba"), lax.axis_index("col")
    barrier = pltpu.get_barrier_semaphore()
    for step in range(1, nb):
        pl.semaphore_signal(barrier, inc=1, device_id=(b_me ^ step, c_me), device_id_type=MESH)
    for step in range(1, nc):
        pl.semaphore_signal(barrier, inc=1, device_id=(b_me, c_me ^ step), device_id_type=MESH)

    def spread(chunk, part):
        for step in range(1, nb):
            pltpu.make_async_remote_copy(
                src_ref=pool.at[pl.ds((chunk * nb + (b_me ^ step)) * rows, rows), part],
                dst_ref=slab.at[chunk, b_me, :, part],
                send_sem=out_sems.at[0, chunk],
                recv_sem=in_sems.at[0, chunk],
                device_id=(b_me ^ step, c_me),
                device_id_type=MESH,
            ).start()

    def own_slab(chunk):
        return pltpu.make_async_copy(
            pool.at[pl.ds((chunk * nb + b_me) * rows, rows)], slab.at[chunk, b_me], own_sems.at[0, chunk]
        )

    def own_turned(chunk):
        return pltpu.make_async_copy(
            slab.at[chunk, pl.ds(c_me * ratio, ratio)], turned.at[chunk, c_me], own_sems.at[1, chunk]
        )

    def own_home(chunk):
        return pltpu.make_async_copy(summed.at[chunk, b_me], home.at[chunk, b_me], own_sems.at[2, chunk])

    def turn(chunk):
        for step in range(1, nc):
            level = c_me ^ step
            pltpu.make_async_remote_copy(
                src_ref=slab.at[chunk, pl.ds(level * ratio, ratio)],
                dst_ref=turned.at[chunk, c_me],
                send_sem=out_sems.at[1, chunk],
                recv_sem=in_sems.at[1, chunk],
                device_id=(b_me, level),
                device_id_type=MESH,
            ).start()

    def back(chunk):
        for step in range(1, nb):
            pltpu.make_async_remote_copy(
                src_ref=summed.at[chunk, b_me ^ step],
                dst_ref=home.at[chunk, b_me],
                send_sem=out_sems.at[2, chunk],
                recv_sem=in_sems.at[2, chunk],
                device_id=(b_me ^ step, c_me),
                device_id_type=MESH,
            ).start()

    buffers = (slab, turned, home)
    peers = (nb - 1, nc - 1, nb - 1)

    def arrived(kind, chunk):
        whole = buffers[kind].at[chunk, pl.ds(0, peers[kind])]
        pltpu.make_async_copy(whole, whole, in_sems.at[kind, chunk]).wait()

    def left(kind, chunk):
        whole = buffers[kind].at[chunk, pl.ds(0, peers[kind])]
        pltpu.make_async_copy(whole, whole, out_sems.at[kind, chunk]).wait()

    def add(chunk):
        @pl.loop(0, rows)
        def _(row):
            for level in range(nc):
                other = jnp.concatenate([turned[chunk, level, part, row] for part in range(ratio)], 0)
                flipped = other.astype(F32).T
                for part in range(ratio):
                    block = level * ratio + part
                    kept = slab[chunk, block, row].astype(F32)
                    summed[chunk, block, row] = (kept + flipped[part * bw : (part + 1) * bw]).astype(BF16)

    per = GROUP // rows
    steps = bw // GROUP
    row_c = energy_c[...]

    def gathered(ref, index, block, inner):
        return jnp.concatenate([ref[index * per + n, block, :, inner, :] for n in range(per)], 0)

    def combine(a_step, b_step, block):
        a_inner = pl.ds(pl.multiple_of(a_step * GROUP, GROUP), GROUP)
        b_inner = pl.ds(pl.multiple_of(b_step * GROUP, GROUP), GROUP)
        mine = gathered(summed, b_step, block, a_inner).astype(F32)
        theirs = gathered(home, a_step, block, b_inner).astype(F32)
        both = mine + jnp.swapaxes(theirs, 0, 1)
        base = base_a[pl.ds(pl.multiple_of(block * bw + a_step * GROUP, GROUP), GROUP), :]
        for b in range(GROUP):
            place = b_step * GROUP + b
            below = base - energy_b[place] - row_c
            pool[place * nb + block, a_inner, :] = (both[b] / below).astype(BF16)

    def widen(step):
        for n in range(per):
            arrived(2, step * per + n)
            own_home(step * per + n).wait()

        @pl.loop(0, (2 * step + 1) * nb)
        def _(place):
            cell, block = place // nb, place % nb
            a_step = jnp.where(cell <= step, step, cell - step - 1)
            b_step = jnp.where(cell <= step, cell, step)
            combine(a_step, b_step, block)

    part_width = width // 2
    units = 6
    tiles = bw // GROUP

    def fetch(index):
        unit, tile = index // tiles, index % tiles
        lanes = pl.ds(pl.multiple_of((unit % 2) * part_width, part_width), part_width)
        copies = []
        for side in range(2):
            slot = (index % TURNS) * 2 + side
            source = w_tiles.at[0, unit // 2, pl.ds(tile * GROUP + side * HALF, HALF), :, lanes]
            target = w_slots.at[slot, :, :, pl.ds(0, part_width)]
            copies.append(pltpu.make_async_copy(source, target, w_sems.at[slot]))
        return copies

    def product(unit):
        where = tuple([unit // 2] + [slice(None)] * bits + [slice(None), pl.ds((unit % 2) * part_width, part_width)])

        @pl.loop(0, tiles)
        def _(tile):
            index = unit * tiles + tile
            for copy in fetch(index):
                copy.wait()
            first = tile * GROUP
            entries = jnp.concatenate(
                [pool[pl.ds((first + n) * nb, nb)].reshape(width, cw) for n in range(GROUP)], 1
            )
            slot = (index % TURNS) * 2
            factors = jnp.concatenate(
                [w_slots[slot + side, :, :, :part_width].reshape(HALF * cw, part_width) for side in range(2)], 0
            )
            piece = jnp.dot(entries, factors, preferred_element_type=F32).reshape([2] * bits + [bw, part_width])

            @pl.when(tile == 0)
            def _():
                total[where] = piece

            @pl.when(tile > 0)
            def _():
                total[where] = total[where] + piece

            @pl.when(index + TURNS < units * tiles)
            def _():
                for copy in fetch(index + TURNS):
                    copy.start()

    def bit(place):
        return (b_me // (1 << place)) % 2

    def order(unit):
        return list(range(bits)) if unit % 2 == 0 else [0] + list(range(1, bits))[::-1]

    def region(unit, fixed):
        lanes = pl.ds((unit % 2) * part_width, part_width)
        picks = [fixed.get(place, slice(None)) for place in range(bits)[::-1]]
        return tuple([unit // 2] + picks + [slice(None), lanes])

    def halving(unit, stage):
        done = order(unit)[:stage]
        place = order(unit)[stage]
        fixed = {n: bit(n) for n in done}
        fixed[place] = 1 - bit(place)
        return pltpu.make_async_remote_copy(
            src_ref=total.at[region(unit, fixed)],
            dst_ref=halved[stage].at[unit],
            send_sem=send_sems.at[unit, stage],
            recv_sem=got_sems.at[unit, stage],
            device_id=(b_me ^ (1 << place), c_me),
            device_id_type=MESH,
        )

    def halved_add(unit, stage):
        halving(unit, stage).wait_recv()
        where = region(unit, {n: bit(n) for n in order(unit)[: stage + 1]})
        total[where] = total[where] + halved[stage][unit]

    levels = nc // 2

    def deal(unit, n):
        level = (unit % 2) * levels + n
        return level, pltpu.make_async_remote_copy(
            src_ref=dealt.at[unit, n],
            dst_ref=spread_out.at[unit // 2, c_me],
            send_sem=send_sems.at[unit, bits + n],
            recv_sem=got_sems.at[unit // 2, bits],
            device_id=(b_me, level),
            device_id_type=MESH,
        )

    def deal_blocks(unit):
        block = total[region(unit, {place: bit(place) for place in range(bits)})]
        for n in range(levels):
            dealt[unit, n] = block[:, n * cw : (n + 1) * cw]

    def deal_start(unit):
        for n in range(levels):
            level, copy = deal(unit, n)
            pl.when(level != c_me)(copy.start)

    def deal_sent(unit):
        for n in range(levels):
            level, copy = deal(unit, n)
            pl.when(level != c_me)(copy.wait_send)

    def finish(unit):
        @pl.when(c_me // levels == unit % 2)
        def _():
            landed = spread_out.at[unit // 2, pl.ds(0, nc - 1)]
            pltpu.make_async_copy(landed, landed, got_sems.at[unit // 2, bits]).wait()
            result = dealt[unit, c_me % levels]
            for step in range(1, nc):
                result = result + spread_out[unit // 2, c_me ^ step]
            sigma[unit // 2] = result

    def pass_on(chunk):
        arrived(0, chunk)
        own_slab(chunk).wait()
        turn(chunk)
        own_turned(chunk).start()

    ahead = FIRST // (nb * rows)
    passes = ((0, ahead), (ahead, chunks - ahead))

    def cube_fetch(group, side, pair):
        slot = side * 3 + pair
        source = w_tiles.at[0, pair, pl.ds(group * GROUP + side * HALF, HALF)]
        return pltpu.make_async_copy(source, w_slots.at[slot], w_sems.at[slot])

    def cube_pass(number):
        start, count = passes[number]
        base, height = start * nb * rows, count * nb * rows
        last = number == len(passes) - 1

        @pl.loop(0, tiles)
        def _(group):
            for side in range(2):
                for pair in range(3):
                    cube_fetch(group, side, pair).wait()
                for n in range(0, HALF, 2):
                    value = None
                    for pair in range(3):
                        factors = w_slots[side * 3 + pair, n : n + 2].reshape(2 * cw, width)
                        term = lax.dot_general(
                            r_rows[pair, base : base + height],
                            factors,
                            (((1,), (1,)), ((), ())),
                            preferred_element_type=F32,
                        )
                        value = term if value is None else value + term
                    at = (side * HALF + n) * cw
                    raw[:height, at : at + 2 * cw] = value
                for pair in range(3):
                    if last:
                        pl.when(group + 1 < tiles)(cube_fetch(group + 1, side, pair).start)
                    else:
                        cube_fetch((group + 1) % tiles, side, pair).start()
            inner = pl.ds(pl.multiple_of(group * GROUP, GROUP), GROUP)

            @pl.loop(0, height // GROUP)
            def _(place):
                entries = raw[pl.ds(pl.multiple_of(place * GROUP, GROUP), GROUP), :]
                split = jnp.stack([entries[:, n * cw : (n + 1) * cw] for n in range(GROUP)], 0)
                pool[pl.ds(base + place * GROUP, GROUP), inner, :] = jnp.swapaxes(split, 0, 1).astype(BF16)

            if number == 0:

                @pl.when(group == 0)
                def _():
                    pl.semaphore_wait(barrier, nb + nc - 2)

                for chunk in range(start, start + count):
                    spread(chunk, inner)
            else:

                @pl.when(group == 0)
                def _():
                    for chunk in range(start):
                        pass_on(chunk)

        if number > 0:

            @pl.loop(start, start + count)
            def _(chunk):
                spread(chunk, pl.ds(0, bw))

        @pl.loop(start, start + count)
        def _(chunk):
            own_slab(chunk).start()

    for side in range(2):
        for pair in range(3):
            cube_fetch(0, side, pair).start()
    for number in range(len(passes)):
        cube_pass(number)
    for index in range(TURNS):
        for copy in fetch(index):
            copy.start()

    @pl.loop(ahead, chunks)
    def _(chunk):
        own_slab(chunk).wait()

    def settle(chunk):
        arrived(1, chunk)
        own_turned(chunk).wait()
        add(chunk)
        back(chunk)
        own_home(chunk).start()

    for chunk in range(chunks):
        if chunk >= ahead:
            arrived(0, chunk)
            turn(chunk)
            own_turned(chunk).start()
        if chunk > 0:
            settle(chunk - 1)
        for step in range(steps - 1):
            if chunk == chunks - 1 - max(1, per // 2) * (steps - 2 - step):
                if step == 0:
                    for number in range(chunks):
                        left(0, number)
                widen(step)
    settle(chunks - 1)
    widen(steps - 1)

    for time in range(units + bits + 1):
        if time < units:
            product(time)
        for stage in range(bits):
            if 0 <= time - stage - 1 < units:
                halved_add(time - stage - 1, stage)
        if 0 <= time - bits < units:
            deal_blocks(time - bits)
        for stage in range(bits):
            if 0 <= time - stage < units:
                halving(time - stage, stage).start()
        if 0 <= time - bits < units:
            deal_start(time - bits)
        if 0 <= time - bits - 1 < units:
            finish(time - bits - 1)
    for unit in range(units):
        for stage in range(bits):
            halving(unit, stage).wait_send()
        deal_sent(unit)

    @pl.loop(0, chunks)
    def _(chunk):
        for kind in range(1, 3):
            left(kind, chunk)


def doubles(r_rows, w_tiles, base_a, energy_b, energy_c, nb, nc):
    bw, cw, width = w_tiles.shape[2:]
    chunks, rows = CHUNKS, bw // CHUNKS
    bits = nb.bit_length() - 1
    block = (rows, bw, cw)
    vmem = pl.BlockSpec(memory_space=pltpu.VMEM)
    hbm = pl.BlockSpec(memory_space=pl.ANY)
    return pl.pallas_call(
        functools.partial(whole_kernel, nb, nc, chunks),
        out_shape=jax.ShapeDtypeStruct((3, bw, cw), F32),
        in_specs=[vmem, hbm, vmem, pl.BlockSpec(memory_space=pltpu.SMEM), vmem],
        out_specs=vmem,
        scratch_shapes=[
            pltpu.VMEM((chunks, nb) + block, BF16),
            pltpu.VMEM((chunks, nc, nb // nc) + block, BF16),
            pltpu.VMEM((chunks, nb) + block, BF16),
            pltpu.VMEM((chunks, nb) + block, BF16),
            pltpu.VMEM((width, bw, cw), BF16),
            pltpu.VMEM((6, HALF, cw, width), BF16),
            pltpu.VMEM((width - FIRST, GROUP * cw), F32),
            pltpu.VMEM((3,) + (2,) * bits + (bw, width), F32),
        ]
        + [pltpu.VMEM((6,) + (2,) * (bits - 1 - stage) + (bw, width // 2), F32) for stage in range(bits)]
        + [
            pltpu.VMEM((6, nc // 2, bw, cw), F32),
            pltpu.VMEM((3, nc, bw, cw), F32),
            pltpu.SemaphoreType.DMA((3, chunks)),
            pltpu.SemaphoreType.DMA((3, chunks)),
            pltpu.SemaphoreType.DMA((3, chunks)),
            pltpu.SemaphoreType.DMA((6,)),
            pltpu.SemaphoreType.DMA((6, bits + nc // 2)),
            pltpu.SemaphoreType.DMA((6, bits + 1)),
        ],
        compiler_params=pltpu.CompilerParams(
            collective_id=0, has_side_effects=True, vmem_limit_bytes=60 << 20
        ),
    )(r_rows, w_tiles, base_a, energy_b, energy_c)


def on_device(r_pairs, w_tiles, virt_energy, energy_shift):
    width = w_tiles.shape[4]
    bw, cw = w_tiles.shape[2], w_tiles.shape[3]
    nb, nc = lax.axis_size("ba"), lax.axis_size("col")
    energy_b = lax.dynamic_slice_in_dim(virt_energy, lax.axis_index("ba") * bw, bw)
    energy_c = lax.dynamic_slice_in_dim(virt_energy, lax.axis_index("col") * cw, cw)
    base_a = jnp.broadcast_to((energy_shift - virt_energy)[:, None], (width, cw))
    r_rows = r_pairs[0].reshape(3, nb, CHUNKS, bw // CHUNKS, width).swapaxes(1, 2).reshape(3, width, width)
    return doubles(r_rows, w_tiles, base_a, energy_b, energy_c[None], nb, nc)[None]


def solution(mesh):
    in_specs = (P(), P(None, None, "ba", "col", None), P(), P())
    out_specs = P(None, None, "ba", "col")
    return jax.shard_map(
        on_device, mesh=mesh, in_specs=in_specs, out_specs=out_specs, check_vma=False
    )
```

```python
import functools

import jax
import jax.numpy as jnp
from jax import lax
from jax.experimental import pallas as pl
from jax.experimental.pallas import tpu as pltpu
from jax.sharding import PartitionSpec as P

MESH = pl.DeviceIdType.MESH
CHUNKS = 16
GROUP = 16
HALF = 8
TURNS = 3
BF16, F32 = jnp.bfloat16, jnp.float32


def whole_kernel(nb, nc, chunks, *refs):
    r_pairs, w_tiles, energy, energy_rows, shift, sigma = refs[:6]
    slab, turned, summed, home, pool, r_rows, base_a, w_slots, raw, total = refs[6:16]
    paired, gathered_in, dealt, spread_out = refs[16:20]
    out_sems, in_sems, own_sems, w_sems, r_sems, send_sems, got_sems = refs[20:]
    rows, bw, cw = slab.shape[2:]
    width = nb * bw
    ratio = nb // nc
    chips, per, steps = nb // 2, GROUP // rows, bw // GROUP
    b_me, c_me = lax.axis_index("ba"), lax.axis_index("col")
    barrier = pltpu.get_barrier_semaphore()
    for step in range(1, nb):
        pl.semaphore_signal(barrier, inc=1, device_id=(b_me ^ step, c_me), device_id_type=MESH)
    for step in range(1, nc):
        pl.semaphore_signal(barrier, inc=1, device_id=(b_me, c_me ^ step), device_id_type=MESH)

    def block_rows(chunk, block):
        return pl.ds((chunk // per * nb + block) * GROUP + chunk % per * rows, rows)

    def spread(chunk, part):
        for step in range(1, nb):
            pltpu.make_async_remote_copy(
                src_ref=pool.at[block_rows(chunk, b_me ^ step), part],
                dst_ref=slab.at[chunk, b_me, :, part],
                send_sem=out_sems.at[0, chunk],
                recv_sem=in_sems.at[0, chunk],
                device_id=(b_me ^ step, c_me),
                device_id_type=MESH,
            ).start()

    def own_slab(chunk):
        return pltpu.make_async_copy(
            pool.at[block_rows(chunk, b_me)], slab.at[chunk, b_me], own_sems.at[0, chunk]
        )

    def own_turned(chunk):
        return pltpu.make_async_copy(
            slab.at[chunk, pl.ds(c_me * ratio, ratio)], turned.at[chunk, c_me], own_sems.at[1, chunk]
        )

    def own_home(chunk):
        return pltpu.make_async_copy(summed.at[chunk, b_me], home.at[chunk, b_me], own_sems.at[2, chunk])

    def turn(chunk):
        for step in range(1, nc):
            level = c_me ^ step
            pltpu.make_async_remote_copy(
                src_ref=slab.at[chunk, pl.ds(level * ratio, ratio)],
                dst_ref=turned.at[chunk, c_me],
                send_sem=out_sems.at[1, chunk],
                recv_sem=in_sems.at[1, chunk],
                device_id=(b_me, level),
                device_id_type=MESH,
            ).start()

    def back(chunk):
        for step in range(1, nb):
            pltpu.make_async_remote_copy(
                src_ref=summed.at[chunk, b_me ^ step],
                dst_ref=home.at[chunk, b_me],
                send_sem=out_sems.at[2, chunk],
                recv_sem=in_sems.at[2, chunk],
                device_id=(b_me ^ step, c_me),
                device_id_type=MESH,
            ).start()

    buffers = (slab, turned, home)
    peers = (nb - 1, nc - 1, nb - 1)

    def arrived(kind, chunk):
        whole = buffers[kind].at[chunk, pl.ds(0, peers[kind])]
        pltpu.make_async_copy(whole, whole, in_sems.at[kind, chunk]).wait()

    def left(kind, chunk):
        whole = buffers[kind].at[chunk, pl.ds(0, peers[kind])]
        pltpu.make_async_copy(whole, whole, out_sems.at[kind, chunk]).wait()

    def add(chunk):
        @pl.loop(0, rows)
        def _(row):
            for level in range(nc):
                other = jnp.concatenate([turned[chunk, level, part, row] for part in range(ratio)], 0)
                flipped = other.astype(F32).T
                for part in range(ratio):
                    block = level * ratio + part
                    kept = slab[chunk, block, row].astype(F32)
                    summed[chunk, block, row] = (kept + flipped[part * bw : (part + 1) * bw]).astype(BF16)

    row_c = energy_rows[pl.ds(c_me, 1), :]

    def gathered(ref, index, block, inner):
        return jnp.concatenate([ref[index * per + n, block, :, inner, :] for n in range(per)], 0)

    def combine(a_step, b_step, block):
        a_inner = pl.ds(pl.multiple_of(a_step * GROUP, GROUP), GROUP)
        b_inner = pl.ds(pl.multiple_of(b_step * GROUP, GROUP), GROUP)
        mine = gathered(summed, b_step, block, a_inner).astype(F32)
        theirs = gathered(home, a_step, block, b_inner).astype(F32)
        both = mine + jnp.swapaxes(theirs, 0, 1)
        base = base_a[pl.ds(pl.multiple_of(block * bw + a_step * GROUP, GROUP), GROUP), :]
        for b in range(GROUP):
            place = b_step * GROUP + b
            below = base - energy[b_me * bw + place] - row_c
            pool[place * nb + block, a_inner, :] = (both[b] / below).astype(BF16)

    def widen(step):
        for n in range(per):
            arrived(2, step * per + n)
            own_home(step * per + n).wait()

        @pl.loop(0, (2 * step + 1) * nb)
        def _(place):
            cell, block = place // nb, place % nb
            a_step = jnp.where(cell <= step, step, cell - step - 1)
            b_step = jnp.where(cell <= step, cell, step)
            combine(a_step, b_step, block)

    part_width = width // 2
    units = 6
    tiles = bw // GROUP

    def fetch(index):
        unit, tile = index // tiles, index % tiles
        lanes = pl.ds(pl.multiple_of((unit % 2) * part_width, part_width), part_width)
        copies = []
        for side in range(2):
            slot = (index % TURNS) * 2 + side
            source = w_tiles.at[0, unit // 2, pl.ds(tile * GROUP + side * HALF, HALF), :, lanes]
            target = w_slots.at[slot, :, :, pl.ds(0, part_width)]
            copies.append(pltpu.make_async_copy(source, target, w_sems.at[slot]))
        return copies

    def lanes_of(unit):
        return pl.ds((unit % 2) * part_width, part_width)

    def product(unit):
        where = (unit // 2, slice(None), slice(None), slice(None), lanes_of(unit))

        @pl.loop(0, tiles)
        def _(tile):
            index = unit * tiles + tile
            for copy in fetch(index):
                copy.wait()
            first = tile * GROUP
            entries = jnp.concatenate(
                [pool[pl.ds((first + n) * nb, nb)].reshape(width, cw) for n in range(GROUP)], 1
            )
            slot = (index % TURNS) * 2
            factors = jnp.concatenate(
                [w_slots[slot + side, :, :, :part_width].reshape(HALF * cw, part_width) for side in range(2)], 0
            )
            piece = jnp.dot(entries, factors, preferred_element_type=F32).reshape(chips, 2, bw, part_width)

            @pl.when(tile == 0)
            def _():
                total[where] = piece

            @pl.when(tile > 0)
            def _():
                total[where] = total[where] + piece

            @pl.when(index + TURNS < units * tiles)
            def _():
                for copy in fetch(index + TURNS):
                    copy.start()

    core, chip = b_me % 2, b_me // 2

    def pair_up(unit):
        return pltpu.make_async_remote_copy(
            src_ref=total.at[unit // 2, :, 1 - core, :, lanes_of(unit)],
            dst_ref=paired.at[unit],
            send_sem=send_sems.at[unit, 0],
            recv_sem=got_sems.at[unit, 0],
            device_id=(b_me ^ 1, c_me),
            device_id_type=MESH,
        )

    def pair_add(unit):
        pair_up(unit).wait_recv()
        where = (unit // 2, slice(None), core, slice(None), lanes_of(unit))
        total[where] = total[where] + paired[unit]

    def gather_in(unit):
        for step in range(1, chips):
            pltpu.make_async_remote_copy(
                src_ref=total.at[unit // 2, chip ^ step, core, :, lanes_of(unit)],
                dst_ref=gathered_in.at[unit, chip],
                send_sem=send_sems.at[unit, 1],
                recv_sem=got_sems.at[unit, 1],
                device_id=(b_me ^ (2 * step), c_me),
                device_id_type=MESH,
            ).start()

    def wait_blocks(unit, sem):
        blocks = gathered_in.at[unit, pl.ds(0, chips - 1)]
        pltpu.make_async_copy(blocks, blocks, sem).wait()

    levels = nc // 2

    def deal(unit, n):
        level = (unit % 2) * levels + n
        return level, pltpu.make_async_remote_copy(
            src_ref=dealt.at[unit, n],
            dst_ref=spread_out.at[unit // 2, c_me],
            send_sem=send_sems.at[unit, 2 + n],
            recv_sem=got_sems.at[unit // 2, 2],
            device_id=(b_me, level),
            device_id_type=MESH,
        )

    def deal_blocks(unit):
        wait_blocks(unit, got_sems.at[unit, 1])
        block = total[unit // 2, chip, core, :, lanes_of(unit)]
        for step in range(1, chips):
            block = block + gathered_in[unit, chip ^ step]
        for n in range(levels):
            dealt[unit, n] = block[:, n * cw : (n + 1) * cw]

    def deal_start(unit):
        for n in range(levels):
            level, copy = deal(unit, n)
            pl.when(level != c_me)(copy.start)

    def deal_sent(unit):
        for n in range(levels):
            level, copy = deal(unit, n)
            pl.when(level != c_me)(copy.wait_send)

    def finish(unit):
        @pl.when(c_me // levels == unit % 2)
        def _():
            landed = spread_out.at[unit // 2, pl.ds(0, nc - 1)]
            pltpu.make_async_copy(landed, landed, got_sems.at[unit // 2, 2]).wait()
            result = dealt[unit, c_me % levels]
            for step in range(1, nc):
                result = result + spread_out[unit // 2, c_me ^ step]
            sigma[unit // 2] = result

    def pass_on(chunk):
        arrived(0, chunk)
        own_slab(chunk).wait()
        turn(chunk)
        own_turned(chunk).start()

    passes = ((0, 1), (1, steps))
    early = min(2, per)

    def cube_fetch(group, side, pair):
        slot = side * 3 + pair
        source = w_tiles.at[0, pair, pl.ds(group * GROUP + side * HALF, HALF)]
        return pltpu.make_async_copy(source, w_slots.at[slot], w_sems.at[slot])

    def cube_pass(number):
        first, stop = passes[number]
        base, height = first * nb * GROUP, (stop - first) * nb * GROUP
        last = number == len(passes) - 1

        @pl.loop(0, tiles)
        def _(group):
            for side in range(2):
                for pair in range(3):
                    cube_fetch(group, side, pair).wait()
                for n in range(0, HALF, 2):
                    value = None
                    for pair in range(3):
                        factors = w_slots[side * 3 + pair, n : n + 2].reshape(2 * cw, width)
                        term = lax.dot_general(
                            r_rows[pair, first:stop].reshape(height, width),
                            factors,
                            (((1,), (1,)), ((), ())),
                            preferred_element_type=F32,
                        )
                        value = term if value is None else value + term
                    at = (side * HALF + n) * cw
                    raw[:height, at : at + 2 * cw] = value
                for pair in range(3):
                    if last:
                        pl.when(group + 1 < tiles)(cube_fetch(group + 1, side, pair).start)
                    else:
                        cube_fetch((group + 1) % tiles, side, pair).start()
            inner = pl.ds(pl.multiple_of(group * GROUP, GROUP), GROUP)

            @pl.loop(0, height // GROUP)
            def _(place):
                entries = raw[pl.ds(pl.multiple_of(place * GROUP, GROUP), GROUP), :]
                split = jnp.stack([entries[:, n * cw : (n + 1) * cw] for n in range(GROUP)], 0)
                pool[pl.ds(base + place * GROUP, GROUP), inner, :] = jnp.swapaxes(split, 0, 1).astype(BF16)

            if number == 0:

                @pl.when(group == 0)
                def _():
                    pl.semaphore_wait(barrier, nb + nc - 2)

                spread(0, inner)
            else:
                for chunk in range(early):

                    @pl.when(group == chunk * tiles // early)
                    def _():
                        pass_on(chunk)

        @pl.loop(max(first * per, 1), stop * per)
        def _(chunk):
            spread(chunk, pl.ds(0, bw))

        @pl.loop(first * per, stop * per)
        def _(chunk):
            own_slab(chunk).start()

    def r_fetch(pair, step):
        return pltpu.make_async_copy(r_pairs.at[pair, :, step], r_rows.at[pair, step], r_sems.at[pair, step])

    for step in range(steps):
        for pair in range(3):
            r_fetch(pair, step).start()
            if step == 0:
                for side in range(2):
                    cube_fetch(0, side, pair).start()
    for level in range(nc):
        row = jnp.broadcast_to(energy_rows[level : level + 1, :], (cw, cw))
        base_a[level * cw : (level + 1) * cw, :] = shift[0] - row.T
    for number in range(len(passes)):
        for step in range(*passes[number]):
            for pair in range(3):
                r_fetch(pair, step).wait()
        cube_pass(number)
    for index in range(TURNS):
        for copy in fetch(index):
            copy.start()

    @pl.loop(early, chunks)
    def _(chunk):
        own_slab(chunk).wait()

    def settle(chunk):
        arrived(1, chunk)
        own_turned(chunk).wait()
        add(chunk)
        back(chunk)
        own_home(chunk).start()

    for chunk in range(chunks):
        if chunk >= early:
            arrived(0, chunk)
            turn(chunk)
            own_turned(chunk).start()
        if chunk > 0:
            settle(chunk - 1)
        for step in range(steps - 1):
            if chunk == chunks - 1 - max(1, per // 2) * (steps - 2 - step):
                if step == 0:
                    for number in range(chunks):
                        left(0, number)
                widen(step)
    settle(chunks - 1)
    widen(steps - 1)

    for time in range(units + 3):
        if time < units:
            product(time)
        if 0 <= time - 1 < units:
            pair_add(time - 1)
        if 0 <= time - 2 < units:
            deal_blocks(time - 2)
        if time < units:
            pair_up(time).start()
        if 0 <= time - 1 < units:
            gather_in(time - 1)
        if 0 <= time - 2 < units:
            deal_start(time - 2)
        if 0 <= time - 3:
            finish(time - 3)
    for unit in range(units):
        pair_up(unit).wait_send()
        wait_blocks(unit, send_sems.at[unit, 1])
        deal_sent(unit)

    @pl.loop(0, chunks)
    def _(chunk):
        for kind in range(1, 3):
            left(kind, chunk)


def doubles(r_pairs, w_tiles, energy, shift, nb, nc):
    bw, cw, width = w_tiles.shape[2:]
    chunks, rows = CHUNKS, bw // CHUNKS
    steps = bw // GROUP
    block = (rows, bw, cw)
    vmem, smem = pl.BlockSpec(memory_space=pltpu.VMEM), pl.BlockSpec(memory_space=pltpu.SMEM)
    hbm = pl.BlockSpec(memory_space=pl.ANY)
    return pl.pallas_call(
        functools.partial(whole_kernel, nb, nc, chunks),
        out_shape=jax.ShapeDtypeStruct((3, bw, cw), F32),
        in_specs=[hbm, hbm, smem, vmem, smem],
        out_specs=vmem,
        scratch_shapes=[
            pltpu.VMEM((chunks, nb) + block, BF16),
            pltpu.VMEM((chunks, nc, nb // nc) + block, BF16),
            pltpu.VMEM((chunks, nb) + block, BF16),
            pltpu.VMEM((chunks, nb) + block, BF16),
            pltpu.VMEM((width, bw, cw), BF16),
            pltpu.VMEM((3, steps, nb, GROUP, width), BF16),
            pltpu.VMEM((width, cw), F32),
            pltpu.VMEM((6, HALF, cw, width), BF16),
            pltpu.VMEM((width - nb * GROUP, GROUP * cw), F32),
            pltpu.VMEM((3, nb // 2, 2, bw, width), F32),
            pltpu.VMEM((6, nb // 2, bw, width // 2), F32),
            pltpu.VMEM((6, nb // 2, bw, width // 2), F32),
            pltpu.VMEM((6, nc // 2, bw, cw), F32),
            pltpu.VMEM((3, nc, bw, cw), F32),
            pltpu.SemaphoreType.DMA((3, chunks)),
            pltpu.SemaphoreType.DMA((3, chunks)),
            pltpu.SemaphoreType.DMA((3, chunks)),
            pltpu.SemaphoreType.DMA((6,)),
            pltpu.SemaphoreType.DMA((3, steps)),
            pltpu.SemaphoreType.DMA((6, 2 + nc // 2)),
            pltpu.SemaphoreType.DMA((6, 3)),
        ],
        compiler_params=pltpu.CompilerParams(
            collective_id=0, has_side_effects=True, vmem_limit_bytes=60 << 20
        ),
    )(r_pairs.reshape(3, nb, steps, GROUP, width), w_tiles, energy, energy.reshape(nc, cw), shift)


def on_device(r_pairs, w_tiles, virt_energy, energy_shift):
    nb, nc = lax.axis_size("ba"), lax.axis_size("col")
    return doubles(r_pairs, w_tiles, virt_energy, energy_shift, nb, nc)[None]


def solution(mesh):
    in_specs = (P(), P(None, None, "ba", "col", None), P(), P())
    out_specs = P(None, None, "ba", "col")
    return jax.shard_map(
        on_device, mesh=mesh, in_specs=in_specs, out_specs=out_specs, check_vma=False
    )
```

```python
import functools

import jax
import jax.numpy as jnp
from jax import lax
from jax.experimental import pallas as pl
from jax.experimental.pallas import tpu as pltpu
from jax.sharding import PartitionSpec as P

MESH = pl.DeviceIdType.MESH
CHUNKS = 16
GROUP = 16
HALF = 8
TURNS = 3
AHEAD = 2
BF16, F32 = jnp.bfloat16, jnp.float32


def whole_kernel(nb, nc, chunks, *refs):
    r_pairs, w_tiles, energy, energy_rows, shift, sigma = refs[:6]
    slab, turned, summed, home, pool, r_rows, base_a, w_slots, raw, total = refs[6:16]
    paired, gathered_in, late_in, dealt, spread_out = refs[16:21]
    out_sems, in_sems, own_sems, w_sems, r_sems, send_sems, got_sems = refs[21:]
    rows, bw, cw = slab.shape[2:]
    width = nb * bw
    ratio = nb // nc
    chips, per, steps = nb // 2, GROUP // rows, bw // GROUP
    b_me, c_me = lax.axis_index("ba"), lax.axis_index("col")
    barrier = pltpu.get_barrier_semaphore()
    for step in range(1, nb):
        pl.semaphore_signal(barrier, inc=1, device_id=(b_me ^ step, c_me), device_id_type=MESH)
    for step in range(1, nc):
        pl.semaphore_signal(barrier, inc=1, device_id=(b_me, c_me ^ step), device_id_type=MESH)

    def block_rows(chunk, block):
        return pl.ds((chunk // per * nb + block) * GROUP + chunk % per * rows, rows)

    def spread(chunk, part):
        for step in range(1, nb):
            pltpu.make_async_remote_copy(
                src_ref=pool.at[block_rows(chunk, b_me ^ step), part],
                dst_ref=slab.at[chunk, b_me, :, part],
                send_sem=out_sems.at[0, chunk],
                recv_sem=in_sems.at[0, chunk],
                device_id=(b_me ^ step, c_me),
                device_id_type=MESH,
            ).start()

    def own_slab(chunk):
        return pltpu.make_async_copy(
            pool.at[block_rows(chunk, b_me)], slab.at[chunk, b_me], own_sems.at[0, chunk]
        )

    def own_turned(chunk):
        return pltpu.make_async_copy(
            slab.at[chunk, pl.ds(c_me * ratio, ratio)], turned.at[chunk, c_me], own_sems.at[1, chunk]
        )

    def own_home(chunk):
        return pltpu.make_async_copy(summed.at[chunk, b_me], home.at[chunk, b_me], own_sems.at[2, chunk])

    def turn(chunk):
        for step in range(1, nc):
            level = c_me ^ step
            pltpu.make_async_remote_copy(
                src_ref=slab.at[chunk, pl.ds(level * ratio, ratio)],
                dst_ref=turned.at[chunk, c_me],
                send_sem=out_sems.at[1, chunk],
                recv_sem=in_sems.at[1, chunk],
                device_id=(b_me, level),
                device_id_type=MESH,
            ).start()

    def back(chunk):
        for step in range(1, nb):
            pltpu.make_async_remote_copy(
                src_ref=summed.at[chunk, b_me ^ step],
                dst_ref=home.at[chunk, b_me],
                send_sem=out_sems.at[2, chunk],
                recv_sem=in_sems.at[2, chunk],
                device_id=(b_me ^ step, c_me),
                device_id_type=MESH,
            ).start()

    buffers = (slab, turned, home)
    peers = (nb - 1, nc - 1, nb - 1)

    def arrived(kind, chunk):
        whole = buffers[kind].at[chunk, pl.ds(0, peers[kind])]
        pltpu.make_async_copy(whole, whole, in_sems.at[kind, chunk]).wait()

    def left(kind, chunk):
        whole = buffers[kind].at[chunk, pl.ds(0, peers[kind])]
        pltpu.make_async_copy(whole, whole, out_sems.at[kind, chunk]).wait()

    def add(chunk):
        @pl.loop(0, rows)
        def _(row):
            for level in range(nc):
                other = jnp.concatenate([turned[chunk, level, part, row] for part in range(ratio)], 0)
                flipped = other.astype(F32).T
                for part in range(ratio):
                    block = level * ratio + part
                    kept = slab[chunk, block, row].astype(F32)
                    summed[chunk, block, row] = (kept + flipped[part * bw : (part + 1) * bw]).astype(BF16)

    row_c = energy_rows[pl.ds(c_me, 1), :]

    def gathered(ref, index, block, inner):
        return jnp.concatenate([ref[index * per + n, block, :, inner, :] for n in range(per)], 0)

    def combine(a_step, b_step, block):
        a_inner = pl.ds(pl.multiple_of(a_step * GROUP, GROUP), GROUP)
        b_inner = pl.ds(pl.multiple_of(b_step * GROUP, GROUP), GROUP)
        mine = gathered(summed, b_step, block, a_inner).astype(F32)
        theirs = gathered(home, a_step, block, b_inner).astype(F32)
        both = mine + jnp.swapaxes(theirs, 0, 1)
        base = base_a[pl.ds(pl.multiple_of(block * bw + a_step * GROUP, GROUP), GROUP), :]
        for b in range(GROUP):
            place = b_step * GROUP + b
            below = base - energy[b_me * bw + place] - row_c
            pool[place * nb + block, a_inner, :] = (both[b] / below).astype(BF16)

    def came_home(step):
        for n in range(per):
            arrived(2, step * per + n)
            own_home(step * per + n).wait()

    def widen(step):
        came_home(step)

        @pl.loop(0, (2 * step + 1) * nb)
        def _(place):
            cell, block = place // nb, place % nb
            a_step = jnp.where(cell <= step, step, cell - step - 1)
            b_step = jnp.where(cell <= step, cell, step)
            combine(a_step, b_step, block)

    def widen_last_b():
        @pl.loop(0, (steps - 1) * nb)
        def _(place):
            combine(place // nb, steps - 1, place % nb)

    def widen_last_a():
        came_home(steps - 1)

        @pl.loop(0, steps * nb)
        def _(place):
            combine(steps - 1, place // nb, place % nb)

    part_width = width // 2
    units = 6
    tiles = steps
    before = units * (steps - 1)
    items = before + units + units * steps
    levels = nc // 2
    core, chip = b_me % 2, b_me // 2
    parts = (pl.ds(0, bw - GROUP), pl.ds(bw - GROUP, GROUP))
    heights = (bw - GROUP, GROUP)

    def item(index):
        late = index - before - units
        unit = jnp.where(
            index < before, index // (steps - 1), jnp.where(late < 0, index - before, late // steps)
        )
        tile = jnp.where(index < before, index % (steps - 1), jnp.where(late < 0, steps - 1, late % steps))
        return unit, tile

    def lanes_of(unit):
        return pl.ds(pl.multiple_of((unit % 2) * part_width, part_width), part_width)

    def fetch(index):
        unit, tile = item(index)
        copies = []
        for side in range(2):
            slot = (index % TURNS) * 2 + side
            source = w_tiles.at[0, unit // 2, pl.ds(tile * GROUP + side * HALF, HALF), :, lanes_of(unit)]
            target = w_slots.at[slot, :, :, pl.ds(0, part_width)]
            copies.append(pltpu.make_async_copy(source, target, w_sems.at[slot]))
        return copies

    def multiply(index, unit, tile, part):
        for copy in fetch(index):
            copy.wait()
        first = tile * GROUP
        entries = jnp.concatenate(
            [pool[pl.ds((first + n) * nb, nb), parts[part]].reshape(nb * heights[part], cw) for n in range(GROUP)], 1
        )
        slot = (index % TURNS) * 2
        factors = jnp.concatenate(
            [w_slots[slot + side, :, :, :part_width].reshape(HALF * cw, part_width) for side in range(2)], 0
        )
        piece = jnp.dot(entries, factors, preferred_element_type=F32).reshape(chips, 2, heights[part], part_width)
        where = (unit // 2, slice(None), slice(None), parts[part], lanes_of(unit))

        @pl.when(tile == 0)
        def _():
            total[where] = piece

        @pl.when(tile > 0)
        def _():
            total[where] = total[where] + piece

        @pl.when(index + TURNS < items)
        def _():
            for copy in fetch(index + TURNS):
                copy.start()

    def pair_up(unit):
        return pltpu.make_async_remote_copy(
            src_ref=total.at[unit // 2, :, 1 - core, parts[0], lanes_of(unit)],
            dst_ref=paired.at[unit, :, parts[0]],
            send_sem=send_sems.at[0, unit, 0],
            recv_sem=got_sems.at[0, unit, 0],
            device_id=(b_me ^ 1, c_me),
            device_id_type=MESH,
        )

    def pair_add(unit):
        pair_up(unit).wait_recv()
        where = (unit // 2, slice(None), core, parts[0], lanes_of(unit))
        total[where] = total[where] + paired[unit, :, parts[0]]

    def gather_in(unit):
        for step in range(1, chips):
            pltpu.make_async_remote_copy(
                src_ref=total.at[unit // 2, chip ^ step, core, parts[0], lanes_of(unit)],
                dst_ref=gathered_in.at[unit, chip, parts[0]],
                send_sem=send_sems.at[0, unit, 1],
                recv_sem=got_sems.at[0, unit, 1],
                device_id=(b_me ^ (2 * step), c_me),
                device_id_type=MESH,
            ).start()

    def wait_blocks(part, unit, sem):
        blocks = (gathered_in.at[unit, pl.ds(0, chips - 1), parts[0]], late_in.at[unit, pl.ds(0, nb - 1)])[part]
        pltpu.make_async_copy(blocks, blocks, sem).wait()

    def scatter(unit):
        for step in range(1, nb):
            peer = b_me ^ step
            pltpu.make_async_remote_copy(
                src_ref=total.at[unit // 2, peer // 2, peer % 2, parts[1], lanes_of(unit)],
                dst_ref=late_in.at[unit, b_me],
                send_sem=send_sems.at[1, unit, 1],
                recv_sem=got_sems.at[1, unit, 1],
                device_id=(peer, c_me),
                device_id_type=MESH,
            ).start()

    def deal(part, unit, n):
        level = (unit % 2) * levels + n
        return level, pltpu.make_async_remote_copy(
            src_ref=dealt.at[unit, n, parts[part]],
            dst_ref=spread_out.at[unit // 2, c_me, parts[part]],
            send_sem=send_sems.at[part, unit, 2 + n],
            recv_sem=got_sems.at[part, unit // 2, 2],
            device_id=(b_me, level),
            device_id_type=MESH,
        )

    def deal_blocks(part, unit):
        wait_blocks(part, unit, got_sems.at[part, unit, 1])
        block = total[unit // 2, chip, core, parts[part], lanes_of(unit)]
        if part == 0:
            for step in range(1, chips):
                block = block + gathered_in[unit, chip ^ step, parts[0]]
        else:
            for step in range(1, nb):
                block = block + late_in[unit, b_me ^ step]
        for n in range(levels):
            dealt[unit, n, parts[part]] = block[:, n * cw : (n + 1) * cw]

    def deal_start(part, unit):
        for n in range(levels):
            level, copy = deal(part, unit, n)
            pl.when(level != c_me)(copy.start)

    def deal_sent(part, unit):
        for n in range(levels):
            level, copy = deal(part, unit, n)
            pl.when(level != c_me)(copy.wait_send)

    def finish(part, unit):
        @pl.when(c_me // levels == unit % 2)
        def _():
            landed = spread_out.at[unit // 2, pl.ds(0, nc - 1), parts[part]]
            pltpu.make_async_copy(landed, landed, got_sems.at[part, unit // 2, 2]).wait()
            result = dealt[unit, c_me % levels, parts[part]]
            for step in range(1, nc):
                result = result + spread_out[unit // 2, c_me ^ step, parts[part]]
            sigma[unit // 2, parts[part]] = result

    def pass_on(chunk):
        arrived(0, chunk)
        own_slab(chunk).wait()
        turn(chunk)
        own_turned(chunk).start()

    passes = ((0, 1), (1, steps))
    early = min(2, per)

    def cube_fetch(group, side, pair):
        slot = side * 3 + pair
        source = w_tiles.at[0, pair, pl.ds(group * GROUP + side * HALF, HALF)]
        return pltpu.make_async_copy(source, w_slots.at[slot], w_sems.at[slot])

    def cube_pass(number):
        first, stop = passes[number]
        base, height = first * nb * GROUP, (stop - first) * nb * GROUP
        last = number == len(passes) - 1

        @pl.loop(0, tiles)
        def _(group):
            for side in range(2):
                for pair in range(3):
                    cube_fetch(group, side, pair).wait()
                for n in range(0, HALF, 2):
                    value = None
                    for pair in range(3):
                        factors = w_slots[side * 3 + pair, n : n + 2].reshape(2 * cw, width)
                        term = lax.dot_general(
                            r_rows[pair, first:stop].reshape(height, width),
                            factors,
                            (((1,), (1,)), ((), ())),
                            preferred_element_type=F32,
                        )
                        value = term if value is None else value + term
                    at = (side * HALF + n) * cw
                    raw[:height, at : at + 2 * cw] = value
                for pair in range(3):
                    if last:
                        pl.when(group + 1 < tiles)(cube_fetch(group + 1, side, pair).start)
                    else:
                        cube_fetch((group + 1) % tiles, side, pair).start()
            inner = pl.ds(pl.multiple_of(group * GROUP, GROUP), GROUP)

            @pl.loop(0, height // GROUP)
            def _(place):
                entries = raw[pl.ds(pl.multiple_of(place * GROUP, GROUP), GROUP), :]
                split = jnp.stack([entries[:, n * cw : (n + 1) * cw] for n in range(GROUP)], 0)
                pool[pl.ds(base + place * GROUP, GROUP), inner, :] = jnp.swapaxes(split, 0, 1).astype(BF16)

            if number == 0:

                @pl.when(group == 0)
                def _():
                    pl.semaphore_wait(barrier, nb + nc - 2)

                spread(0, inner)
            else:
                for chunk in range(early):

                    @pl.when(group == chunk * tiles // early)
                    def _():
                        pass_on(chunk)

        @pl.loop(max(first * per, 1), stop * per)
        def _(chunk):
            spread(chunk, pl.ds(0, bw))

        @pl.loop(first * per, stop * per)
        def _(chunk):
            own_slab(chunk).start()

    def r_fetch(pair, step):
        return pltpu.make_async_copy(r_pairs.at[pair, :, step], r_rows.at[pair, step], r_sems.at[pair, step])

    for step in range(steps):
        for pair in range(3):
            r_fetch(pair, step).start()
            if step == 0:
                for side in range(2):
                    cube_fetch(0, side, pair).start()
    for level in range(nc):
        row = jnp.broadcast_to(energy_rows[level : level + 1, :], (cw, cw))
        base_a[level * cw : (level + 1) * cw, :] = shift[0] - row.T
    for number in range(len(passes)):
        for step in range(*passes[number]):
            for pair in range(3):
                r_fetch(pair, step).wait()
        cube_pass(number)
    for index in range(TURNS):
        for copy in fetch(index):
            copy.start()

    @pl.loop(early, chunks)
    def _(chunk):
        own_slab(chunk).wait()

    def settle(chunk):
        arrived(1, chunk)
        own_turned(chunk).wait()
        add(chunk)
        back(chunk)
        own_home(chunk).start()

    for chunk in range(chunks):
        for later in (range(early, AHEAD + 1) if chunk == 0 else (chunk + AHEAD,)):
            if later < chunks:
                arrived(0, later)
                turn(later)
                own_turned(later).start()
        if chunk > 0:
            settle(chunk - 1)
        for step in range(steps - 1):
            if chunk == chunks - 2 - max(1, per // 2) * (steps - 2 - step):
                if step == 0:
                    for number in range(chunks):
                        left(0, number)
                widen(step)
        if chunk >= chunks - 2:
            half = before // 2
            begin = half * (chunk - chunks + 2)

            @pl.loop(begin, begin + half)
            def _(index):
                multiply(index, index // (steps - 1), index % (steps - 1), 0)

    settle(chunks - 1)
    widen_last_b()

    @pl.loop(0, units)
    def _(unit):
        multiply(before + unit, unit, steps - 1, 0)
        pair_up(unit).start()

    @pl.loop(0, units)
    def _(unit):
        pair_add(unit)
        gather_in(unit)

    widen_last_a()

    for time in range(units + 2):
        if time < units:

            @pl.loop(0, tiles)
            def _(tile):
                multiply(before + units + time * tiles + tile, time, tile, 1)

        if time < units:
            deal_blocks(0, time)
        if 0 <= time - 2 < units:
            deal_blocks(1, time - 2)
        if time < units:
            scatter(time)
            deal_start(0, time)
        if 0 <= time - 2 < units:
            deal_start(1, time - 2)
    for unit in range(units):
        for part in range(2):
            finish(part, unit)

    @pl.loop(0, units)
    def _(unit):
        pair_up(unit).wait_send()
        for part in range(2):
            wait_blocks(part, unit, send_sems.at[part, unit, 1])
            deal_sent(part, unit)

    @pl.loop(0, chunks)
    def _(chunk):
        for kind in range(1, 3):
            left(kind, chunk)


def doubles(r_pairs, w_tiles, energy, shift, nb, nc):
    bw, cw, width = w_tiles.shape[2:]
    chunks, rows = CHUNKS, bw // CHUNKS
    steps = bw // GROUP
    block = (rows, bw, cw)
    vmem, smem = pl.BlockSpec(memory_space=pltpu.VMEM), pl.BlockSpec(memory_space=pltpu.SMEM)
    hbm = pl.BlockSpec(memory_space=pl.ANY)
    return pl.pallas_call(
        functools.partial(whole_kernel, nb, nc, chunks),
        out_shape=jax.ShapeDtypeStruct((3, bw, cw), F32),
        in_specs=[hbm, hbm, smem, vmem, smem],
        out_specs=vmem,
        scratch_shapes=[
            pltpu.VMEM((chunks, nb) + block, BF16),
            pltpu.VMEM((chunks, nc, nb // nc) + block, BF16),
            pltpu.VMEM((chunks, nb) + block, BF16),
            pltpu.VMEM((chunks, nb) + block, BF16),
            pltpu.VMEM((width, bw, cw), BF16),
            pltpu.VMEM((3, steps, nb, GROUP, width), BF16),
            pltpu.VMEM((width, cw), F32),
            pltpu.VMEM((6, HALF, cw, width), BF16),
            pltpu.VMEM((width - nb * GROUP, GROUP * cw), F32),
            pltpu.VMEM((3, nb // 2, 2, bw, width), F32),
            pltpu.VMEM((6, nb // 2, bw, width // 2), F32),
            pltpu.VMEM((6, nb // 2, bw, width // 2), F32),
            pltpu.VMEM((6, nb, GROUP, width // 2), F32),
            pltpu.VMEM((6, nc // 2, bw, cw), F32),
            pltpu.VMEM((3, nc, bw, cw), F32),
            pltpu.SemaphoreType.DMA((3, chunks)),
            pltpu.SemaphoreType.DMA((3, chunks)),
            pltpu.SemaphoreType.DMA((3, chunks)),
            pltpu.SemaphoreType.DMA((6,)),
            pltpu.SemaphoreType.DMA((3, steps)),
            pltpu.SemaphoreType.DMA((2, 6, 2 + nc // 2)),
            pltpu.SemaphoreType.DMA((2, 6, 3)),
        ],
        compiler_params=pltpu.CompilerParams(
            collective_id=0, has_side_effects=True, vmem_limit_bytes=60 << 20
        ),
    )(r_pairs.reshape(3, nb, steps, GROUP, width), w_tiles, energy, energy.reshape(nc, cw), shift)


def on_device(r_pairs, w_tiles, virt_energy, energy_shift):
    nb, nc = lax.axis_size("ba"), lax.axis_size("col")
    return doubles(r_pairs, w_tiles, virt_energy, energy_shift, nb, nc)[None]


def solution(mesh):
    in_specs = (P(), P(None, None, "ba", "col", None), P(), P())
    out_specs = P(None, None, "ba", "col")
    return jax.shard_map(
        on_device, mesh=mesh, in_specs=in_specs, out_specs=out_specs, check_vma=False
    )
```

```python
import functools

import jax
import jax.numpy as jnp
from jax import lax
from jax.experimental import pallas as pl
from jax.experimental.pallas import tpu as pltpu
from jax.sharding import PartitionSpec as P

MESH = pl.DeviceIdType.MESH
CHUNKS = 16
GROUP = 16
HALF = 8
TURNS = 3
AHEAD = 2
LANES = 128
BF16, F32 = jnp.bfloat16, jnp.float32


def whole_kernel(nb, nc, chunks, *refs):
    r_pairs, w_tiles, energy, energy_rows, shift, sigma = refs[:6]
    slab, turned, summed, home, pool, r_rows, base_a, w_slots, raw, total = refs[6:16]
    paired, gathered_in, late_in, dealt, spread_out = refs[16:21]
    out_sems, in_sems, own_sems, w_sems, held_sems, r_sems, send_sems, got_sems = refs[21:]
    rows, bw, cw = slab.shape[2:]
    width = nb * bw
    ratio = nb // nc
    chips, per, steps = nb // 2, GROUP // rows, bw // GROUP
    b_me, c_me = lax.axis_index("ba"), lax.axis_index("col")
    barrier = pltpu.get_barrier_semaphore()
    for step in range(1, nb):
        pl.semaphore_signal(barrier, inc=1, device_id=(b_me ^ step, c_me), device_id_type=MESH)
    for step in range(1, nc):
        pl.semaphore_signal(barrier, inc=1, device_id=(b_me, c_me ^ step), device_id_type=MESH)

    def block_rows(chunk, block):
        return pl.ds((chunk // per * nb + block) * GROUP + chunk % per * rows, rows)

    def spread(chunk, part):
        for step in range(1, nb):
            pltpu.make_async_remote_copy(
                src_ref=pool.at[block_rows(chunk, b_me ^ step), part],
                dst_ref=slab.at[chunk, b_me, :, part],
                send_sem=out_sems.at[0, chunk],
                recv_sem=in_sems.at[0, chunk],
                device_id=(b_me ^ step, c_me),
                device_id_type=MESH,
            ).start()

    def own_slab(chunk):
        return pltpu.make_async_copy(
            pool.at[block_rows(chunk, b_me)], slab.at[chunk, b_me], own_sems.at[0, chunk]
        )

    def own_turned(chunk):
        return pltpu.make_async_copy(
            slab.at[chunk, pl.ds(c_me * ratio, ratio)], turned.at[chunk, c_me], own_sems.at[1, chunk]
        )

    def own_home(chunk):
        return pltpu.make_async_copy(summed.at[chunk, b_me], home.at[chunk, b_me], own_sems.at[2, chunk])

    def turn(chunk):
        for step in range(1, nc):
            level = c_me ^ step
            pltpu.make_async_remote_copy(
                src_ref=slab.at[chunk, pl.ds(level * ratio, ratio)],
                dst_ref=turned.at[chunk, c_me],
                send_sem=out_sems.at[1, chunk],
                recv_sem=in_sems.at[1, chunk],
                device_id=(b_me, level),
                device_id_type=MESH,
            ).start()

    def back(chunk):
        for step in range(1, nb):
            pltpu.make_async_remote_copy(
                src_ref=summed.at[chunk, b_me ^ step],
                dst_ref=home.at[chunk, b_me],
                send_sem=out_sems.at[2, chunk],
                recv_sem=in_sems.at[2, chunk],
                device_id=(b_me ^ step, c_me),
                device_id_type=MESH,
            ).start()

    buffers = (slab, turned, home)
    peers = (nb - 1, nc - 1, nb - 1)

    def arrived(kind, chunk):
        whole = buffers[kind].at[chunk, pl.ds(0, peers[kind])]
        pltpu.make_async_copy(whole, whole, in_sems.at[kind, chunk]).wait()

    def left(kind, chunk):
        whole = buffers[kind].at[chunk, pl.ds(0, peers[kind])]
        pltpu.make_async_copy(whole, whole, out_sems.at[kind, chunk]).wait()

    def add(chunk):
        @pl.loop(0, rows)
        def _(row):
            for level in range(nc):
                other = jnp.concatenate([turned[chunk, level, part, row] for part in range(ratio)], 0)
                flipped = other.astype(F32).T
                for part in range(ratio):
                    block = level * ratio + part
                    kept = slab[chunk, block, row].astype(F32)
                    summed[chunk, block, row] = (kept + flipped[part * bw : (part + 1) * bw]).astype(BF16)

    row_c = energy_rows[pl.ds(c_me, 1), :]

    def gathered(ref, index, block, inner):
        return jnp.concatenate([ref[index * per + n, block, :, inner, :] for n in range(per)], 0)

    def combine(a_step, b_step, block):
        a_inner = pl.ds(pl.multiple_of(a_step * GROUP, GROUP), GROUP)
        b_inner = pl.ds(pl.multiple_of(b_step * GROUP, GROUP), GROUP)
        mine = gathered(summed, b_step, block, a_inner).astype(F32)
        theirs = gathered(home, a_step, block, b_inner).astype(F32)
        both = mine + jnp.swapaxes(theirs, 0, 1)
        base = base_a[pl.ds(pl.multiple_of(block * bw + a_step * GROUP, GROUP), GROUP), :]
        for b in range(GROUP):
            place = b_step * GROUP + b
            below = base - energy[b_me * bw + place] - row_c
            pool[place * nb + block, a_inner, :] = (both[b] / below).astype(BF16)

    def came_home(step):
        for n in range(per):
            arrived(2, step * per + n)
            own_home(step * per + n).wait()

    def widen(step):
        came_home(step)

        @pl.loop(0, (2 * step + 1) * nb)
        def _(place):
            cell, block = place // nb, place % nb
            a_step = jnp.where(cell <= step, step, cell - step - 1)
            b_step = jnp.where(cell <= step, cell, step)
            combine(a_step, b_step, block)

    def widen_last_b():
        @pl.loop(0, (steps - 1) * nb)
        def _(place):
            combine(place // nb, steps - 1, place % nb)

    def widen_last_a():
        came_home(steps - 1)

        @pl.loop(0, steps * nb)
        def _(place):
            combine(steps - 1, place // nb, place % nb)

    part_width = width // 2
    units = 6
    tiles = steps
    levels = nc // 2
    core, chip = b_me % 2, b_me // 2
    parts = (pl.ds(0, bw - GROUP), pl.ds(bw - GROUP, GROUP))
    heights = (bw - GROUP, GROUP)

    def lanes_of(unit):
        return pl.ds(pl.multiple_of((unit % 2) * part_width, part_width), part_width)

    def fetch(turn, unit, tile):
        copies = []
        for side in range(2):
            slot = turn * 2 + side
            source = w_tiles.at[0, unit // 2, pl.ds(tile * GROUP + side * HALF, HALF), :, lanes_of(unit)]
            target = w_slots.at[slot, :, :, pl.ds(0, part_width)]
            copies.append(pltpu.make_async_copy(source, target, w_sems.at[slot]))
        return copies

    def fetch_start(turn, unit, tile):
        for copy in fetch(turn, unit, tile):
            copy.start()

    sides = cw // bw
    fits = cw % LANES == 0 and per * sides == nb and sides == 2 and part_width == 2 * cw
    held = chunks if fits else 0

    def held_block(place, plane, block):
        if plane == 0:
            return slab.at[place, block]
        return turned.at[place, block // ratio, block % ratio]

    def hold(place):
        unit, tile = place % units, place // units
        for plane in range(2):
            for block in range(nb):
                source = w_tiles.at[
                    0,
                    unit // 2,
                    pl.ds(tile * GROUP + block // sides * rows, rows),
                    pl.ds(block % sides * bw, bw),
                    pl.ds((unit % 2) * part_width + plane * cw, cw),
                ]
                target = held_block(place, plane, block)
                pltpu.make_async_copy(source, target, held_sems.at[plane, place]).start()

    def held_wait(place):
        for plane, kept in enumerate((slab, turned)):
            whole = kept.at[place]
            pltpu.make_async_copy(whole, whole, held_sems.at[plane, place]).wait()

    def held_factors(place):
        planes = []
        for plane in range(2):
            blocks = [held_block(place, plane, block)[...] for block in range(nb)]
            planes.append(
                jnp.concatenate([blocks[n // rows * sides + side][n % rows] for n in range(GROUP) for side in range(sides)], 0)
            )
        return jnp.concatenate(planes, 1)

    def slot_factors(turn):
        return jnp.concatenate(
            [w_slots[turn * 2 + side, :, :, :part_width].reshape(HALF * cw, part_width) for side in range(2)], 0
        )

    def multiply(factors, unit, tile, part):
        entries = jnp.concatenate(
            [
                pool[(tile * GROUP + n) * nb : (tile * GROUP + n + 1) * nb, parts[part]].reshape(
                    nb * heights[part], cw
                )
                for n in range(GROUP)
            ],
            1,
        )
        piece = jnp.dot(entries, factors, preferred_element_type=F32).reshape(chips, 2, heights[part], part_width)
        where = (unit // 2, slice(None), slice(None), parts[part], lanes_of(unit))
        if tile == 0:
            total[where] = piece
        else:
            total[where] = total[where] + piece

    def fetched(turn, unit, tile):
        for copy in fetch(turn, unit, tile):
            copy.wait()
        return slot_factors(turn)

    flowing = [tile for tile in range(steps - 1) if (tile + 1) * units > held]

    def early_place(index, begin):
        return begin + index // len(flowing), flowing[index % len(flowing)]

    def early_start(begin):
        for index in range(TURNS):
            fetch_start(index, *early_place(index, begin))

    def early_units(begin, stop):
        if len(flowing) == 1:

            @pl.loop(begin, stop)
            def _(unit):
                for tile in range(steps - 1):
                    if tile in flowing:
                        multiply(fetched(unit - begin, unit, tile), unit, tile, 0)

                        @pl.when(unit + TURNS < units)
                        def _():
                            fetch_start(unit - begin, unit + TURNS, tile)
                    else:
                        held_wait(tile * units + unit)
                        multiply(held_factors(tile * units + unit), unit, tile, 0)
        else:
            for index in range((stop - begin) * len(flowing)):
                unit, tile = early_place(index, begin)
                multiply(fetched(index % TURNS, unit, tile), unit, tile, 0)
                later, place = early_place(index + TURNS, begin)
                if later < units:
                    fetch_start(index % TURNS, later, place)

    def last_b_start():
        for index in range(TURNS):
            fetch_start(index, index, steps - 1)

    def last_b_units():
        @pl.loop(0, units // TURNS)
        def _(lap):
            for turn in range(TURNS):
                unit = lap * TURNS + turn
                multiply(fetched(turn, unit, steps - 1), unit, steps - 1, 0)

                @pl.when(unit + TURNS < units)
                def _():
                    fetch_start(turn, unit + TURNS, steps - 1)

                pair_up(unit).start()

    stream = [(unit, tile) for unit in range(units) for tile in range(tiles) if tile * units + unit >= held]

    def late_start():
        for index in range(TURNS):
            fetch_start(index, *stream[index])

    def late_unit(unit):
        for tile in range(tiles):
            place = tile * units + unit
            if place < held:
                if tile in flowing or tile == steps - 1:
                    held_wait(place)
                multiply(held_factors(place), unit, tile, 1)
            else:
                index = stream.index((unit, tile))
                multiply(fetched(index % TURNS, unit, tile), unit, tile, 1)
                if index + TURNS < len(stream):
                    fetch_start(index % TURNS, *stream[index + TURNS])

    def pair_up(unit):
        return pltpu.make_async_remote_copy(
            src_ref=total.at[unit // 2, :, 1 - core, parts[0], lanes_of(unit)],
            dst_ref=paired.at[unit, :, parts[0]],
            send_sem=send_sems.at[0, unit, 0],
            recv_sem=got_sems.at[0, unit, 0],
            device_id=(b_me ^ 1, c_me),
            device_id_type=MESH,
        )

    def pair_add(unit):
        pair_up(unit).wait_recv()
        where = (unit // 2, slice(None), core, parts[0], lanes_of(unit))
        total[where] = total[where] + paired[unit, :, parts[0]]

    def gather_in(unit):
        for step in range(1, chips):
            pltpu.make_async_remote_copy(
                src_ref=total.at[unit // 2, chip ^ step, core, parts[0], lanes_of(unit)],
                dst_ref=gathered_in.at[unit, chip, parts[0]],
                send_sem=send_sems.at[0, unit, 1],
                recv_sem=got_sems.at[0, unit, 1],
                device_id=(b_me ^ (2 * step), c_me),
                device_id_type=MESH,
            ).start()

    def late_pair(unit):
        return pltpu.make_async_remote_copy(
            src_ref=total.at[unit // 2, :, 1 - core, parts[1], lanes_of(unit)],
            dst_ref=paired.at[unit, :, parts[1]],
            send_sem=send_sems.at[1, unit, 0],
            recv_sem=got_sems.at[1, unit, 0],
            device_id=(b_me ^ 1, c_me),
            device_id_type=MESH,
        )

    def late_add(unit):
        late_pair(unit).wait_recv()
        where = (unit // 2, slice(None), core, parts[1], lanes_of(unit))
        total[where] = total[where] + paired[unit, :, parts[1]]

    def wait_blocks(part, unit, sem):
        blocks = (gathered_in.at[unit, pl.ds(0, chips - 1), parts[0]], late_in.at[unit, pl.ds(0, chips - 1)])[part]
        pltpu.make_async_copy(blocks, blocks, sem).wait()

    def scatter(unit):
        for step in range(1, chips):
            pltpu.make_async_remote_copy(
                src_ref=total.at[unit // 2, chip ^ step, core, parts[1], lanes_of(unit)],
                dst_ref=late_in.at[unit, chip],
                send_sem=send_sems.at[1, unit, 1],
                recv_sem=got_sems.at[1, unit, 1],
                device_id=(b_me ^ (2 * step), c_me),
                device_id_type=MESH,
            ).start()

    def deal(part, unit, n):
        level = (unit % 2) * levels + n
        return level, pltpu.make_async_remote_copy(
            src_ref=dealt.at[unit, n, parts[part]],
            dst_ref=spread_out.at[unit // 2, c_me, parts[part]],
            send_sem=send_sems.at[part, unit, 2 + n],
            recv_sem=got_sems.at[part, unit // 2, 2],
            device_id=(b_me, level),
            device_id_type=MESH,
        )

    def deal_blocks(part, unit):
        wait_blocks(part, unit, got_sems.at[part, unit, 1])
        block = total[unit // 2, chip, core, parts[part], lanes_of(unit)]
        if part == 0:
            for step in range(1, chips):
                block = block + gathered_in[unit, chip ^ step, parts[0]]
        else:
            for step in range(1, chips):
                block = block + late_in[unit, chip ^ step]
        for n in range(levels):
            dealt[unit, n, parts[part]] = block[:, n * cw : (n + 1) * cw]

    def deal_start(part, unit):
        for n in range(levels):
            level, copy = deal(part, unit, n)
            pl.when(level != c_me)(copy.start)

    def deal_sent(part, unit):
        for n in range(levels):
            level, copy = deal(part, unit, n)
            pl.when(level != c_me)(copy.wait_send)

    def finish(part, unit):
        @pl.when(c_me // levels == unit % 2)
        def _():
            landed = spread_out.at[unit // 2, pl.ds(0, nc - 1), parts[part]]
            pltpu.make_async_copy(landed, landed, got_sems.at[part, unit // 2, 2]).wait()
            result = dealt[unit, c_me % levels, parts[part]]
            for step in range(1, nc):
                result = result + spread_out[unit // 2, c_me ^ step, parts[part]]
            sigma[unit // 2, parts[part]] = result

    def pass_on(chunk):
        arrived(0, chunk)
        own_slab(chunk).wait()
        turn(chunk)
        own_turned(chunk).start()

    passes = ((0, 1), (1, steps))
    early = min(2, per)

    def cube_fetch(group, side, pair):
        slot = side * 3 + pair
        source = w_tiles.at[0, pair, pl.ds(group * GROUP + side * HALF, HALF)]
        return pltpu.make_async_copy(source, w_slots.at[slot], w_sems.at[slot])

    def cube_pass(number):
        first, stop = passes[number]
        base, height = first * nb * GROUP, (stop - first) * nb * GROUP
        last = number == len(passes) - 1

        @pl.loop(0, tiles)
        def _(group):
            for side in range(2):
                for pair in range(3):
                    cube_fetch(group, side, pair).wait()
                for n in range(0, HALF, 2):
                    value = None
                    for pair in range(3):
                        factors = w_slots[side * 3 + pair, n : n + 2].reshape(2 * cw, width)
                        term = lax.dot_general(
                            r_rows[pair, first:stop].reshape(height, width),
                            factors,
                            (((1,), (1,)), ((), ())),
                            preferred_element_type=F32,
                        )
                        value = term if value is None else value + term
                    at = (side * HALF + n) * cw
                    raw[:height, at : at + 2 * cw] = value
                for pair in range(3):
                    if last:
                        pl.when(group + 1 < tiles)(cube_fetch(group + 1, side, pair).start)
                    else:
                        cube_fetch((group + 1) % tiles, side, pair).start()
            inner = pl.ds(pl.multiple_of(group * GROUP, GROUP), GROUP)

            @pl.loop(0, height // GROUP)
            def _(place):
                entries = raw[pl.ds(pl.multiple_of(place * GROUP, GROUP), GROUP), :]
                split = jnp.stack([entries[:, n * cw : (n + 1) * cw] for n in range(GROUP)], 0)
                pool[pl.ds(base + place * GROUP, GROUP), inner, :] = jnp.swapaxes(split, 0, 1).astype(BF16)

            if number == 0:

                @pl.when(group == 0)
                def _():
                    pl.semaphore_wait(barrier, nb + nc - 2)

                spread(0, inner)
            else:
                for chunk in range(early):

                    @pl.when(group == chunk * tiles // early)
                    def _():
                        pass_on(chunk)

        @pl.loop(max(first * per, 1), stop * per)
        def _(chunk):
            spread(chunk, pl.ds(0, bw))

        @pl.loop(first * per, stop * per)
        def _(chunk):
            own_slab(chunk).start()

    def r_fetch(pair, step):
        return pltpu.make_async_copy(r_pairs.at[pair, :, step], r_rows.at[pair, step], r_sems.at[pair, step])

    for step in range(steps):
        for pair in range(3):
            r_fetch(pair, step).start()
            if step == 0:
                for side in range(2):
                    cube_fetch(0, side, pair).start()
    for level in range(nc):
        row = jnp.broadcast_to(energy_rows[level : level + 1, :], (cw, cw))
        base_a[level * cw : (level + 1) * cw, :] = shift[0] - row.T
    for number in range(len(passes)):
        for step in range(*passes[number]):
            for pair in range(3):
                r_fetch(pair, step).wait()
        cube_pass(number)
    early_start(0)

    @pl.loop(early, chunks)
    def _(chunk):
        own_slab(chunk).wait()

    def settle(chunk):
        arrived(1, chunk)
        own_turned(chunk).wait()
        add(chunk)
        back(chunk)
        own_home(chunk).start()

    for chunk in range(chunks):
        for later in (range(early, AHEAD + 1) if chunk == 0 else (chunk + AHEAD,)):
            if later < chunks:
                arrived(0, later)
                turn(later)
                own_turned(later).start()
        if chunk > 0:
            settle(chunk - 1)
        if chunk > 1:
            left(1, chunk - 2)
            if chunk - 2 < held:
                hold(chunk - 2)
        for step in range(steps - 1):
            if chunk == chunks - 2 - max(1, per // 2) * (steps - 2 - step):
                if step == 0:
                    for number in range(chunks):
                        left(0, number)
                widen(step)
        if chunk >= chunks - 2:
            half = units // 2
            early_units(half * (chunk - chunks + 2), half * (chunk - chunks + 3))
    last_b_start()
    settle(chunks - 1)
    for chunk in range(chunks - 2, chunks):
        left(1, chunk)
        if chunk < held:
            hold(chunk)
    widen_last_b()

    last_b_units()
    late_start()

    @pl.loop(0, units)
    def _(unit):
        pair_add(unit)
        gather_in(unit)

    widen_last_a()

    for unit in range(units):
        late_unit(unit)
        if unit > 0:
            late_add(unit - 1)
            deal_blocks(0, unit - 1)
        late_pair(unit).start()
        if unit > 0:
            scatter(unit - 1)
            deal_start(0, unit - 1)
    late_add(units - 1)
    deal_blocks(0, units - 1)
    scatter(units - 1)
    deal_start(0, units - 1)
    for unit in range(units):
        deal_blocks(1, unit)
        deal_start(1, unit)
    for unit in range(units):
        for part in range(2):
            finish(part, unit)

    @pl.loop(0, units)
    def _(unit):
        pair_up(unit).wait_send()
        late_pair(unit).wait_send()
        for part in range(2):
            wait_blocks(part, unit, send_sems.at[part, unit, 1])
            deal_sent(part, unit)

    @pl.loop(0, chunks)
    def _(chunk):
        left(2, chunk)


def doubles(r_pairs, w_tiles, energy, shift, nb, nc):
    bw, cw, width = w_tiles.shape[2:]
    chunks, rows = CHUNKS, bw // CHUNKS
    steps = bw // GROUP
    block = (rows, bw, cw)
    vmem, smem = pl.BlockSpec(memory_space=pltpu.VMEM), pl.BlockSpec(memory_space=pltpu.SMEM)
    hbm = pl.BlockSpec(memory_space=pl.ANY)
    return pl.pallas_call(
        functools.partial(whole_kernel, nb, nc, chunks),
        out_shape=jax.ShapeDtypeStruct((3, bw, cw), F32),
        in_specs=[hbm, hbm, smem, vmem, smem],
        out_specs=vmem,
        scratch_shapes=[
            pltpu.VMEM((chunks, nb) + block, BF16),
            pltpu.VMEM((chunks, nc, nb // nc) + block, BF16),
            pltpu.VMEM((chunks, nb) + block, BF16),
            pltpu.VMEM((chunks, nb) + block, BF16),
            pltpu.VMEM((width, bw, cw), BF16),
            pltpu.VMEM((3, steps, nb, GROUP, width), BF16),
            pltpu.VMEM((width, cw), F32),
            pltpu.VMEM((6, HALF, cw, width), BF16),
            pltpu.VMEM((width - nb * GROUP, GROUP * cw), F32),
            pltpu.VMEM((3, nb // 2, 2, bw, width), F32),
            pltpu.VMEM((6, nb // 2, bw, width // 2), F32),
            pltpu.VMEM((6, nb // 2, bw, width // 2), F32),
            pltpu.VMEM((6, nb, GROUP, width // 2), F32),
            pltpu.VMEM((6, nc // 2, bw, cw), F32),
            pltpu.VMEM((3, nc, bw, cw), F32),
            pltpu.SemaphoreType.DMA((3, chunks)),
            pltpu.SemaphoreType.DMA((3, chunks)),
            pltpu.SemaphoreType.DMA((3, chunks)),
            pltpu.SemaphoreType.DMA((6,)),
            pltpu.SemaphoreType.DMA((2, chunks)),
            pltpu.SemaphoreType.DMA((3, steps)),
            pltpu.SemaphoreType.DMA((2, 6, 2 + nc // 2)),
            pltpu.SemaphoreType.DMA((2, 6, 3)),
        ],
        compiler_params=pltpu.CompilerParams(
            collective_id=0, has_side_effects=True, vmem_limit_bytes=60 << 20
        ),
    )(r_pairs.reshape(3, nb, steps, GROUP, width), w_tiles, energy, energy.reshape(nc, cw), shift)


def on_device(r_pairs, w_tiles, virt_energy, energy_shift):
    nb, nc = lax.axis_size("ba"), lax.axis_size("col")
    return doubles(r_pairs, w_tiles, virt_energy, energy_shift, nb, nc)[None]


def solution(mesh):
    in_specs = (P(), P(None, None, "ba", "col", None), P(), P())
    out_specs = P(None, None, "ba", "col")
    return jax.shard_map(
        on_device, mesh=mesh, in_specs=in_specs, out_specs=out_specs, check_vma=False
    )
```

```python
import functools

import jax
import jax.numpy as jnp
from jax import lax
from jax.experimental import pallas as pl
from jax.experimental.pallas import tpu as pltpu
from jax.sharding import PartitionSpec as P

MESH = pl.DeviceIdType.MESH
CHUNKS = 16
GROUP = 16
HALF = 8
TURNS = 3
AHEAD = 2
LANES = 128
BF16, F32 = jnp.bfloat16, jnp.float32


def whole_kernel(nb, nc, chunks, *refs):
    r_pairs, w_tiles, energy, energy_rows, shift, sigma = refs[:6]
    slab, turned, summed, home, pool, r_rows, base_a, w_slots, raw, total = refs[6:16]
    paired, gathered_in, late_in, dealt, spread_out = refs[16:21]
    out_sems, in_sems, own_sems, w_sems, held_sems, r_sems, send_sems, got_sems = refs[21:]
    rows, bw, cw = slab.shape[2:]
    width = nb * bw
    ratio = nb // nc
    chips, per, steps = nb // 2, GROUP // rows, bw // GROUP
    b_me, c_me = lax.axis_index("ba"), lax.axis_index("col")
    barrier = pltpu.get_barrier_semaphore()
    for step in range(1, nb):
        pl.semaphore_signal(barrier, inc=1, device_id=(b_me ^ step, c_me), device_id_type=MESH)
    for step in range(1, nc):
        pl.semaphore_signal(barrier, inc=1, device_id=(b_me, c_me ^ step), device_id_type=MESH)

    def block_rows(chunk, block):
        return pl.ds((chunk // per * nb + block) * GROUP + chunk % per * rows, rows)

    def spread(chunk, part):
        for step in range(1, nb):
            pltpu.make_async_remote_copy(
                src_ref=pool.at[block_rows(chunk, b_me ^ step), part],
                dst_ref=slab.at[chunk, b_me, :, part],
                send_sem=out_sems.at[0, chunk],
                recv_sem=in_sems.at[0, chunk],
                device_id=(b_me ^ step, c_me),
                device_id_type=MESH,
            ).start()

    def own_slab(chunk):
        return pltpu.make_async_copy(
            pool.at[block_rows(chunk, b_me)], slab.at[chunk, b_me], own_sems.at[0, chunk]
        )

    def own_turned(chunk):
        return pltpu.make_async_copy(
            slab.at[chunk, pl.ds(c_me * ratio, ratio)], turned.at[chunk, c_me], own_sems.at[1, chunk]
        )

    def own_home(chunk):
        return pltpu.make_async_copy(summed.at[chunk, b_me], home.at[chunk, b_me], own_sems.at[2, chunk])

    def turn(chunk):
        for step in range(1, nc):
            level = c_me ^ step
            pltpu.make_async_remote_copy(
                src_ref=slab.at[chunk, pl.ds(level * ratio, ratio)],
                dst_ref=turned.at[chunk, c_me],
                send_sem=out_sems.at[1, chunk],
                recv_sem=in_sems.at[1, chunk],
                device_id=(b_me, level),
                device_id_type=MESH,
            ).start()

    def back(chunk):
        for step in range(1, nb):
            pltpu.make_async_remote_copy(
                src_ref=summed.at[chunk, b_me ^ step],
                dst_ref=home.at[chunk, b_me],
                send_sem=out_sems.at[2, chunk],
                recv_sem=in_sems.at[2, chunk],
                device_id=(b_me ^ step, c_me),
                device_id_type=MESH,
            ).start()

    buffers = (slab, turned, home)
    peers = (nb - 1, nc - 1, nb - 1)

    def arrived(kind, chunk):
        whole = buffers[kind].at[chunk, pl.ds(0, peers[kind])]
        pltpu.make_async_copy(whole, whole, in_sems.at[kind, chunk]).wait()

    def left(kind, chunk):
        whole = buffers[kind].at[chunk, pl.ds(0, peers[kind])]
        pltpu.make_async_copy(whole, whole, out_sems.at[kind, chunk]).wait()

    def add(chunk):
        @pl.loop(0, rows)
        def _(row):
            for level in range(nc):
                other = jnp.concatenate([turned[chunk, level, part, row] for part in range(ratio)], 0)
                flipped = other.astype(F32).T
                for part in range(ratio):
                    block = level * ratio + part
                    kept = slab[chunk, block, row].astype(F32)
                    summed[chunk, block, row] = (kept + flipped[part * bw : (part + 1) * bw]).astype(BF16)

    row_c = energy_rows[pl.ds(c_me, 1), :]

    def gathered(ref, index, block, inner):
        return jnp.concatenate([ref[index * per + n, block, :, inner, :] for n in range(per)], 0)

    def combine(a_step, b_step, block):
        a_inner = pl.ds(pl.multiple_of(a_step * GROUP, GROUP), GROUP)
        b_inner = pl.ds(pl.multiple_of(b_step * GROUP, GROUP), GROUP)
        mine = gathered(summed, b_step, block, a_inner).astype(F32)
        theirs = gathered(home, a_step, block, b_inner).astype(F32)
        both = mine + jnp.swapaxes(theirs, 0, 1)
        base = base_a[pl.ds(pl.multiple_of(block * bw + a_step * GROUP, GROUP), GROUP), :]
        for b in range(GROUP):
            place = b_step * GROUP + b
            below = base - energy[b_me * bw + place] - row_c
            pool[place * nb + block, a_inner, :] = (both[b] / below).astype(BF16)

    def came_home(step):
        for n in range(per):
            arrived(2, step * per + n)
            own_home(step * per + n).wait()

    def widen(step):
        came_home(step)

        @pl.loop(0, (2 * step + 1) * nb)
        def _(place):
            cell, block = place // nb, place % nb
            a_step = jnp.where(cell <= step, step, cell - step - 1)
            b_step = jnp.where(cell <= step, cell, step)
            combine(a_step, b_step, block)

    def widen_last_b():
        @pl.loop(0, (steps - 1) * nb)
        def _(place):
            combine(place // nb, steps - 1, place % nb)

    def widen_last_a():
        came_home(steps - 1)

        @pl.loop(0, steps * nb)
        def _(place):
            combine(steps - 1, place // nb, place % nb)

    part_width = width // 2
    units = 6
    tiles = steps
    levels = nc // 2
    core, chip = b_me % 2, b_me // 2
    parts = (pl.ds(0, bw - GROUP), pl.ds(bw - GROUP, GROUP))
    heights = (bw - GROUP, GROUP)

    def lanes_of(unit):
        return pl.ds(pl.multiple_of((unit % 2) * part_width, part_width), part_width)

    def fetch(turn, unit, tile):
        copies = []
        for side in range(2):
            slot = turn * 2 + side
            source = w_tiles.at[0, unit // 2, pl.ds(tile * GROUP + side * HALF, HALF), :, lanes_of(unit)]
            target = w_slots.at[slot, :, :, pl.ds(0, part_width)]
            copies.append(pltpu.make_async_copy(source, target, w_sems.at[slot]))
        return copies

    def fetch_start(turn, unit, tile):
        for copy in fetch(turn, unit, tile):
            copy.start()

    sides = cw // bw
    fits = cw % LANES == 0 and per * sides == nb and sides == 2 and part_width == 2 * cw
    held = chunks if fits else 0

    def held_block(place, plane, block):
        if plane == 0:
            return slab.at[place, block]
        return turned.at[place, block // ratio, block % ratio]

    def hold(place):
        unit, tile = place % units, place // units
        for plane in range(2):
            for block in range(nb):
                source = w_tiles.at[
                    0,
                    unit // 2,
                    pl.ds(tile * GROUP + block // sides * rows, rows),
                    pl.ds(block % sides * bw, bw),
                    pl.ds((unit % 2) * part_width + plane * cw, cw),
                ]
                target = held_block(place, plane, block)
                pltpu.make_async_copy(source, target, held_sems.at[plane, place]).start()

    def held_wait(place):
        for plane, kept in enumerate((slab, turned)):
            whole = kept.at[place]
            pltpu.make_async_copy(whole, whole, held_sems.at[plane, place]).wait()

    def held_factors(place):
        planes = []
        for plane in range(2):
            blocks = [held_block(place, plane, block)[...] for block in range(nb)]
            planes.append(
                jnp.concatenate([blocks[n // rows * sides + side][n % rows] for n in range(GROUP) for side in range(sides)], 0)
            )
        return jnp.concatenate(planes, 1)

    def slot_factors(turn):
        return jnp.concatenate(
            [w_slots[turn * 2 + side, :, :, :part_width].reshape(HALF * cw, part_width) for side in range(2)], 0
        )

    def multiply(factors, unit, tile, part):
        entries = jnp.concatenate(
            [
                pool[(tile * GROUP + n) * nb : (tile * GROUP + n + 1) * nb, parts[part]].reshape(
                    nb * heights[part], cw
                )
                for n in range(GROUP)
            ],
            1,
        )
        piece = jnp.dot(entries, factors, preferred_element_type=F32).reshape(chips, 2, heights[part], part_width)
        where = (unit // 2, slice(None), slice(None), parts[part], lanes_of(unit))
        if tile == 0:
            total[where] = piece
        else:
            total[where] = total[where] + piece

    def fetched(turn, unit, tile):
        for copy in fetch(turn, unit, tile):
            copy.wait()
        return slot_factors(turn)

    flowing = [tile for tile in range(steps - 1) if (tile + 1) * units > held]

    def early_place(index, begin):
        return begin + index // len(flowing), flowing[index % len(flowing)]

    def early_start(begin):
        for index in range(TURNS):
            fetch_start(index, *early_place(index, begin))

    def early_units(begin, stop):
        if len(flowing) == 1:

            @pl.loop(begin, stop)
            def _(unit):
                for tile in range(steps - 1):
                    if tile in flowing:
                        multiply(fetched(unit - begin, unit, tile), unit, tile, 0)

                        @pl.when(unit + TURNS < units)
                        def _():
                            fetch_start(unit - begin, unit + TURNS, tile)
                    else:
                        held_wait(tile * units + unit)
                        multiply(held_factors(tile * units + unit), unit, tile, 0)
        else:
            for index in range((stop - begin) * len(flowing)):
                unit, tile = early_place(index, begin)
                multiply(fetched(index % TURNS, unit, tile), unit, tile, 0)
                later, place = early_place(index + TURNS, begin)
                if later < units:
                    fetch_start(index % TURNS, later, place)

    def last_b_start():
        for index in range(TURNS):
            fetch_start(index, index, steps - 1)

    def last_b_units():
        @pl.loop(0, units // TURNS)
        def _(lap):
            for turn in range(TURNS):
                unit = lap * TURNS + turn
                multiply(fetched(turn, unit, steps - 1), unit, steps - 1, 0)

                @pl.when(unit + TURNS < units)
                def _():
                    fetch_start(turn, unit + TURNS, steps - 1)

                pair_up(unit).start()

                @pl.when(unit > 0)
                def _():
                    pair_add(unit - 1)
                    gather_in(unit - 1)

    stream = [(unit, tile) for unit in range(units) for tile in range(tiles) if tile * units + unit >= held]

    def late_start():
        for index in range(TURNS):
            fetch_start(index, *stream[index])

    def late_unit(unit):
        for tile in range(tiles):
            place = tile * units + unit
            if place < held:
                if tile in flowing or tile == steps - 1:
                    held_wait(place)
                multiply(held_factors(place), unit, tile, 1)
            else:
                index = stream.index((unit, tile))
                multiply(fetched(index % TURNS, unit, tile), unit, tile, 1)
                if index + TURNS < len(stream):
                    fetch_start(index % TURNS, *stream[index + TURNS])

    def pair_up(unit):
        return pltpu.make_async_remote_copy(
            src_ref=total.at[unit // 2, :, 1 - core, parts[0], lanes_of(unit)],
            dst_ref=paired.at[unit, :, parts[0]],
            send_sem=send_sems.at[0, unit, 0],
            recv_sem=got_sems.at[0, unit, 0],
            device_id=(b_me ^ 1, c_me),
            device_id_type=MESH,
        )

    def pair_add(unit):
        pair_up(unit).wait_recv()
        where = (unit // 2, slice(None), core, parts[0], lanes_of(unit))
        total[where] = total[where] + paired[unit, :, parts[0]]

    def gather_in(unit):
        for step in range(1, chips):
            pltpu.make_async_remote_copy(
                src_ref=total.at[unit // 2, chip ^ step, core, parts[0], lanes_of(unit)],
                dst_ref=gathered_in.at[unit, chip, parts[0]],
                send_sem=send_sems.at[0, unit, 1],
                recv_sem=got_sems.at[0, unit, 1],
                device_id=(b_me ^ (2 * step), c_me),
                device_id_type=MESH,
            ).start()

    def late_pair(unit):
        return pltpu.make_async_remote_copy(
            src_ref=total.at[unit // 2, :, 1 - core, parts[1], lanes_of(unit)],
            dst_ref=paired.at[unit, :, parts[1]],
            send_sem=send_sems.at[1, unit, 0],
            recv_sem=got_sems.at[1, unit, 0],
            device_id=(b_me ^ 1, c_me),
            device_id_type=MESH,
        )

    def late_add(unit):
        late_pair(unit).wait_recv()
        where = (unit // 2, slice(None), core, parts[1], lanes_of(unit))
        total[where] = total[where] + paired[unit, :, parts[1]]

    def wait_blocks(part, unit, sem):
        blocks = (gathered_in.at[unit, pl.ds(0, chips - 1), parts[0]], late_in.at[unit, pl.ds(0, chips - 1)])[part]
        pltpu.make_async_copy(blocks, blocks, sem).wait()

    def scatter(unit):
        for step in range(1, chips):
            pltpu.make_async_remote_copy(
                src_ref=total.at[unit // 2, chip ^ step, core, parts[1], lanes_of(unit)],
                dst_ref=late_in.at[unit, chip],
                send_sem=send_sems.at[1, unit, 1],
                recv_sem=got_sems.at[1, unit, 1],
                device_id=(b_me ^ (2 * step), c_me),
                device_id_type=MESH,
            ).start()

    def deal(part, unit, n):
        level = (unit % 2) * levels + n
        return level, pltpu.make_async_remote_copy(
            src_ref=dealt.at[unit, n, parts[part]],
            dst_ref=spread_out.at[unit // 2, c_me, parts[part]],
            send_sem=send_sems.at[part, unit, 2 + n],
            recv_sem=got_sems.at[part, unit // 2, 2],
            device_id=(b_me, level),
            device_id_type=MESH,
        )

    def deal_blocks(part, unit):
        wait_blocks(part, unit, got_sems.at[part, unit, 1])
        block = total[unit // 2, chip, core, parts[part], lanes_of(unit)]
        if part == 0:
            for step in range(1, chips):
                block = block + gathered_in[unit, chip ^ step, parts[0]]
        else:
            for step in range(1, chips):
                block = block + late_in[unit, chip ^ step]
        for n in range(levels):
            dealt[unit, n, parts[part]] = block[:, n * cw : (n + 1) * cw]

    def deal_start(part, unit):
        for n in range(levels):
            level, copy = deal(part, unit, n)
            pl.when(level != c_me)(copy.start)

    def deal_sent(part, unit):
        for n in range(levels):
            level, copy = deal(part, unit, n)
            pl.when(level != c_me)(copy.wait_send)

    def finish(part, unit):
        @pl.when(c_me // levels == unit % 2)
        def _():
            landed = spread_out.at[unit // 2, pl.ds(0, nc - 1), parts[part]]
            pltpu.make_async_copy(landed, landed, got_sems.at[part, unit // 2, 2]).wait()
            result = dealt[unit, c_me % levels, parts[part]]
            for step in range(1, nc):
                result = result + spread_out[unit // 2, c_me ^ step, parts[part]]
            sigma[unit // 2, parts[part]] = result

    def pass_on(chunk):
        arrived(0, chunk)
        own_slab(chunk).wait()
        turn(chunk)
        own_turned(chunk).start()

    passes = ((0, 1), (1, steps))
    early = min(2, per)

    def cube_fetch(group, side, pair):
        slot = side * 3 + pair
        source = w_tiles.at[0, pair, pl.ds(group * GROUP + side * HALF, HALF)]
        return pltpu.make_async_copy(source, w_slots.at[slot], w_sems.at[slot])

    def cube_pass(number):
        first, stop = passes[number]
        base, height = first * nb * GROUP, (stop - first) * nb * GROUP
        last = number == len(passes) - 1

        @pl.loop(0, tiles)
        def _(group):
            for side in range(2):
                for pair in range(3):
                    cube_fetch(group, side, pair).wait()
                for n in range(0, HALF, 2):
                    value = None
                    for pair in range(3):
                        factors = w_slots[side * 3 + pair, n : n + 2].reshape(2 * cw, width)
                        term = lax.dot_general(
                            r_rows[pair, first:stop].reshape(height, width),
                            factors,
                            (((1,), (1,)), ((), ())),
                            preferred_element_type=F32,
                        )
                        value = term if value is None else value + term
                    at = (side * HALF + n) * cw
                    raw[:height, at : at + 2 * cw] = value
                for pair in range(3):
                    if last:
                        pl.when(group + 1 < tiles)(cube_fetch(group + 1, side, pair).start)
                    else:
                        cube_fetch((group + 1) % tiles, side, pair).start()
            inner = pl.ds(pl.multiple_of(group * GROUP, GROUP), GROUP)

            @pl.loop(0, height // GROUP)
            def _(place):
                entries = raw[pl.ds(pl.multiple_of(place * GROUP, GROUP), GROUP), :]
                split = jnp.stack([entries[:, n * cw : (n + 1) * cw] for n in range(GROUP)], 0)
                pool[pl.ds(base + place * GROUP, GROUP), inner, :] = jnp.swapaxes(split, 0, 1).astype(BF16)

            if number == 0:

                @pl.when(group == 0)
                def _():
                    pl.semaphore_wait(barrier, nb + nc - 2)

                spread(0, inner)
            else:
                for chunk in range(early):

                    @pl.when(group == chunk * tiles // early)
                    def _():
                        pass_on(chunk)

        @pl.loop(max(first * per, 1), stop * per)
        def _(chunk):
            spread(chunk, pl.ds(0, bw))

        @pl.loop(first * per, stop * per)
        def _(chunk):
            own_slab(chunk).start()

    def r_fetch(pair, step):
        return pltpu.make_async_copy(r_pairs.at[pair, :, step], r_rows.at[pair, step], r_sems.at[pair, step])

    for step in range(steps):
        for pair in range(3):
            r_fetch(pair, step).start()
            if step == 0:
                for side in range(2):
                    cube_fetch(0, side, pair).start()
    for level in range(nc):
        row = jnp.broadcast_to(energy_rows[level : level + 1, :], (cw, cw))
        base_a[level * cw : (level + 1) * cw, :] = shift[0] - row.T
    for number in range(len(passes)):
        for step in range(*passes[number]):
            for pair in range(3):
                r_fetch(pair, step).wait()
        cube_pass(number)
    early_start(0)

    @pl.loop(early, chunks)
    def _(chunk):
        own_slab(chunk).wait()

    def settle(chunk):
        arrived(1, chunk)
        own_turned(chunk).wait()
        add(chunk)
        back(chunk)
        own_home(chunk).start()

    for chunk in range(chunks):
        for later in (range(early, AHEAD + 1) if chunk == 0 else (chunk + AHEAD,)):
            if later < chunks:
                arrived(0, later)
                turn(later)
                own_turned(later).start()
        if chunk > 0:
            settle(chunk - 1)
        if chunk > 1:
            left(1, chunk - 2)
            if chunk - 2 < held:
                hold(chunk - 2)
        for step in range(steps - 1):
            if chunk == chunks - 2 - max(1, per // 2) * (steps - 2 - step):
                if step == 0:
                    for number in range(chunks):
                        left(0, number)
                widen(step)
        if chunk >= chunks - 2:
            half = units // 2
            early_units(half * (chunk - chunks + 2), half * (chunk - chunks + 3))
    last_b_start()
    settle(chunks - 1)
    for chunk in range(chunks - 2, chunks):
        left(1, chunk)
        if chunk < held:
            hold(chunk)
    widen_last_b()

    last_b_units()
    late_start()

    pair_add(units - 1)
    gather_in(units - 1)

    widen_last_a()

    for unit in range(units):
        late_unit(unit)
        if unit > 0:
            late_add(unit - 1)
            deal_blocks(0, unit - 1)
        late_pair(unit).start()
        if unit > 0:
            scatter(unit - 1)
            deal_start(0, unit - 1)
    late_add(units - 1)
    deal_blocks(0, units - 1)
    scatter(units - 1)
    deal_start(0, units - 1)
    for unit in range(units):
        deal_blocks(1, unit)
        deal_start(1, unit)
    for unit in range(units):
        for part in range(2):
            finish(part, unit)

    @pl.loop(0, units)
    def _(unit):
        pair_up(unit).wait_send()
        late_pair(unit).wait_send()
        for part in range(2):
            wait_blocks(part, unit, send_sems.at[part, unit, 1])
            deal_sent(part, unit)

    @pl.loop(0, chunks)
    def _(chunk):
        left(2, chunk)


def doubles(r_pairs, w_tiles, energy, shift, nb, nc):
    bw, cw, width = w_tiles.shape[2:]
    chunks, rows = CHUNKS, bw // CHUNKS
    steps = bw // GROUP
    block = (rows, bw, cw)
    vmem, smem = pl.BlockSpec(memory_space=pltpu.VMEM), pl.BlockSpec(memory_space=pltpu.SMEM)
    hbm = pl.BlockSpec(memory_space=pl.ANY)
    return pl.pallas_call(
        functools.partial(whole_kernel, nb, nc, chunks),
        out_shape=jax.ShapeDtypeStruct((3, bw, cw), F32),
        in_specs=[hbm, hbm, smem, vmem, smem],
        out_specs=vmem,
        scratch_shapes=[
            pltpu.VMEM((chunks, nb) + block, BF16),
            pltpu.VMEM((chunks, nc, nb // nc) + block, BF16),
            pltpu.VMEM((chunks, nb) + block, BF16),
            pltpu.VMEM((chunks, nb) + block, BF16),
            pltpu.VMEM((width, bw, cw), BF16),
            pltpu.VMEM((3, steps, nb, GROUP, width), BF16),
            pltpu.VMEM((width, cw), F32),
            pltpu.VMEM((6, HALF, cw, width), BF16),
            pltpu.VMEM((width - nb * GROUP, GROUP * cw), F32),
            pltpu.VMEM((3, nb // 2, 2, bw, width), F32),
            pltpu.VMEM((6, nb // 2, bw, width // 2), F32),
            pltpu.VMEM((6, nb // 2, bw, width // 2), F32),
            pltpu.VMEM((6, nb, GROUP, width // 2), F32),
            pltpu.VMEM((6, nc // 2, bw, cw), F32),
            pltpu.VMEM((3, nc, bw, cw), F32),
            pltpu.SemaphoreType.DMA((3, chunks)),
            pltpu.SemaphoreType.DMA((3, chunks)),
            pltpu.SemaphoreType.DMA((3, chunks)),
            pltpu.SemaphoreType.DMA((6,)),
            pltpu.SemaphoreType.DMA((2, chunks)),
            pltpu.SemaphoreType.DMA((3, steps)),
            pltpu.SemaphoreType.DMA((2, 6, 2 + nc // 2)),
            pltpu.SemaphoreType.DMA((2, 6, 3)),
        ],
        compiler_params=pltpu.CompilerParams(
            collective_id=0, has_side_effects=True, vmem_limit_bytes=60 << 20
        ),
    )(r_pairs.reshape(3, nb, steps, GROUP, width), w_tiles, energy, energy.reshape(nc, cw), shift)


def on_device(r_pairs, w_tiles, virt_energy, energy_shift):
    nb, nc = lax.axis_size("ba"), lax.axis_size("col")
    return doubles(r_pairs, w_tiles, virt_energy, energy_shift, nb, nc)[None]


def solution(mesh):
    in_specs = (P(), P(None, None, "ba", "col", None), P(), P())
    out_specs = P(None, None, "ba", "col")
    return jax.shard_map(
        on_device, mesh=mesh, in_specs=in_specs, out_specs=out_specs, check_vma=False
    )
```
